32 devices in a mesh: groups: 2 (over y), cols: 4 (over z), rows: 4 (over x, core).
Axes of the slice: x: 2, y: 2, z: 4, core: 2. Of those that a mesh axis runs over, the one named last changes fastest.
Arguments:
- base_field: float32 [320, 64, 512], P(None, ('groups', 'cols'), 'rows'), parts along dimension 1, may hold values from -6 to 6
- control_field: float32 [320, 64, 512], P(None, ('groups', 'cols', 'rows')), parts along dimension 1, may hold values from -6 to 6
- first_kernel: bfloat16 [9, 320, 320], replicated, may hold values from -0.109375 to 0.109375
- second_kernel: bfloat16 [9, 320, 320], replicated, may hold values from -0.109375 to 0.109375
- control_kernel: bfloat16 [9, 320, 320], replicated, may hold values from -0.109375 to 0.109375
- first_bias: float32 [320], replicated, may hold values from -3 to 3
- second_bias: float32 [320], replicated, may hold values from -3 to 3
- control_bias: float32 [320], replicated, may hold values from -3 to 3
- to_control: bfloat16 [320, 320], replicated, may hold values from -0.3125 to 0.3125
- to_base: bfloat16 [320, 320], replicated, may hold values from -0.3125 to 0.3125
Outputs:
- base_out: float32 [320, 64, 512], P(None, ('groups', 'cols'), 'rows'), parts along dimension 1
- control_out: float32 [320, 64, 512], P(None, ('groups', 'cols', 'rows')), parts along dimension 1
The draws below stay inside these ranges and needn't reach their ends.
There are 2 independent parts, one for each index of `groups`. The reference program is written for one: setup_inputs(seed, part) draws one part's arguments, and reference() takes and returns one part's arrays. A program takes and returns all parts, laid end to end along the dimension named above; an argument that names none is the same for every part. Nothing has to cross between parts.
All inputs are finite; a program needn't handle non-finite values.
Results may differ from the reference program's by a relative error of at most 0.0033.
Values may be sent and summed in bfloat16 or wider, within the bound.
A program may use at most 64 MiB of HBM per device.

```python
import jax
import jax.numpy as jnp

C = 320
WIDTH = 32
HEIGHT = 512


def level_of(own_key, extent, shards, low, high):
    gain, own = 1.0, jax.random.fold_in(own_key, 6)
    for dim, blocks in shards:
        draws = jnp.exp(jax.random.uniform(jax.random.fold_in(own, dim), (blocks,), jnp.float32, low / len(shards), high / len(shards)))
        gain = gain * jnp.repeat(draws, extent[dim] // blocks).reshape([-1 if axis == dim else 1 for axis in range(len(extent))])
    return gain


def normal_values(stream_key, extent, scale, bound, shards=(), held_as=jnp.bfloat16):
    drawn = scale * jax.random.normal(stream_key, extent, jnp.float32)
    if shards:
        drawn = drawn * level_of(stream_key, extent, shards, -0.22, 0.18)
    return jnp.clip(drawn, -bound, bound).astype(held_as)


def setup_inputs(seed: int = 0, part: int = 0) -> dict:
    streams_of = jax.random.split(jax.random.key(seed), 11)
    part_splits = jax.random.split(jax.random.fold_in(streams_of[10], part), 11)
    return {
        "base_field": normal_values(part_splits[0], (C, WIDTH, HEIGHT), 1.0, 6.0, ((1, 4), (2, 4)), jnp.float32),
        "control_field": normal_values(part_splits[1], (C, WIDTH, HEIGHT), 1.0, 6.0, ((1, 16),), jnp.float32),
        "first_kernel": normal_values(streams_of[2], (9, C, C), (9 * C) ** -0.5, 0.109375),
        "second_kernel": normal_values(streams_of[3], (9, C, C), (9 * C) ** -0.5, 0.109375),
        "control_kernel": normal_values(streams_of[4], (9, C, C), (9 * C) ** -0.5, 0.109375),
        "first_bias": normal_values(streams_of[5], (C,), 0.5, 3.0, (), jnp.float32),
        "second_bias": normal_values(streams_of[6], (C,), 0.5, 3.0, (), jnp.float32),
        "control_bias": normal_values(streams_of[7], (C,), 0.5, 3.0, (), jnp.float32),
        "to_control": normal_values(streams_of[8], (C, C), C ** -0.5, 0.3125),
        "to_base": normal_values(streams_of[9], (C, C), C ** -0.5, 0.3125),
    }


def convolve(field, weight, bias):
    padded = jnp.pad(field, ((0, 0), (1, 1), (1, 1))).astype(jnp.float32)
    width = field.shape[1]
    height = field.shape[2]
    total = jnp.zeros((weight.shape[1], width, height), jnp.float32)
    for offset in range(9):
        across = offset // 3
        down = offset % 3
        window = padded[:, across:across + width, down:down + height]
        total = total + jnp.einsum("oc,cwh->owh", weight[offset].astype(jnp.float32), window)
    return total + bias[:, None, None]


def project(matrix, field):
    return jnp.einsum("oc,cwh->owh", matrix.astype(jnp.float32), field.astype(jnp.float32))


def reference(base_field, control_field, first_kernel, second_kernel, control_kernel, first_bias, second_bias, control_bias, to_control, to_base):
    base_round = base_field.astype(jnp.bfloat16)
    hidden = jax.nn.silu(convolve(base_round, first_kernel, first_bias)).astype(jnp.bfloat16)
    base_mid = jax.nn.silu(convolve(hidden, second_kernel, second_bias)) + base_field
    control_round = control_field.astype(jnp.bfloat16)
    control_mid = jax.nn.silu(convolve(control_round, control_kernel, control_bias)) + control_field
    control_out = control_mid + project(to_control, base_mid.astype(jnp.bfloat16))
    base_out = base_mid + project(to_base, control_out.astype(jnp.bfloat16))
    return base_out, control_out
```

```python
import functools

import jax
import jax.numpy as jnp
from jax import lax
from jax.experimental import pallas as pl
from jax.experimental.pallas import tpu as pltpu
from jax.sharding import PartitionSpec as P

MESH = pl.DeviceIdType.MESH
BF = jnp.bfloat16
F32 = jnp.float32
LANE = 128
PACK = 16
SIDES = ((-1, 0), (1, 0), (0, -1), (0, 1), (-1, -1), (1, -1), (-1, 1), (1, 1))
NT = (((1,), (1,)), ((), ()))


def silu(v):
    return 0.5 * v * (1.0 + jnp.tanh(0.5 * v))


def kernel(
    n_cols,
    n_rows,
    base_hbm,
    control_hbm,
    k1_hbm,
    k2_hbm,
    kc_hbm,
    b1_hbm,
    b2_hbm,
    bc_hbm,
    tc_hbm,
    tb_hbm,
    base_new,
    ctl,
    base,
    raw,
    packed,
    shifts_b,
    shifts_h,
    shifts_c,
    row1,
    row2,
    row3,
    biases,
    tc_ref,
    tb_ref,
    edge_out,
    edge_in,
    cedge_out,
    cedge_in,
    strips,
    mid,
    inner_mid,
    bracket,
    arrived,
    load_sem,
    x_send,
    x_recv,
    in_send,
    in_recv,
    ce_send,
    ce_recv,
    fw_send,
    fw_recv,
    out_send,
    out_recv,
):
    C = tc_ref.shape[0]
    tile_cols = base.shape[0] // C
    strip_cols = ctl.shape[2]
    wide = strip_cols * LANE
    main = C - C % LANE
    rest = C - main
    tall = edge_out.shape[2]
    half = n_rows // 2
    half_cols = half * strip_cols
    gid = lax.axis_index("groups")
    k = lax.axis_index("cols")
    r = lax.axis_index("rows")
    lane = lax.broadcasted_iota(jnp.int32, (C, LANE), 1)
    flat = ctl.reshape(n_rows * C * strip_cols, LANE)

    near_base = half * lax.div(r, half)
    far_base = half - near_base
    far_is_left = lax.div(r, half)
    near_start = near_base * strip_cols
    far_start = far_base * strip_cols
    buddies = [near_base + lax.rem(r - near_base + o, half) for o in range(1, half)]
    fars = [far_base + j for j in range(half)]

    def load(i, src, dst):
        copy = pltpu.make_async_copy(src, dst, load_sem.at[i])
        copy.start()
        return copy

    base_load = load(0, base_hbm, base)
    ctl_loads = [
        load(1 + q, control_hbm.at[:, :, pl.ds(q * LANE, LANE)], ctl.at[q]) for q in range(n_rows)
    ]
    more = 1 + n_rows
    weight_loads = [load(more, k1_hbm, raw.at[0])]
    row_loads = [
        load(more + 3 + i, src, dst)
        for i, (src, dst) in enumerate(((b1_hbm, row1), (b2_hbm, row2), (bc_hbm, row3)))
    ]
    weight_loads.append(load(more + 2, kc_hbm, raw.at[2]))
    weight_loads.insert(1, load(more + 1, k2_hbm, raw.at[1]))
    t_loads = [load(more + 6, tc_hbm, tc_ref), load(more + 7, tb_hbm, tb_ref)]

    def there(side):
        dk, dr = side
        ok = None
        for at, step, count in ((k, dk, n_cols), (r, dr, n_rows)):
            if step:
                test = (at > 0) if step < 0 else (at < count - 1)
                ok = test if ok is None else jnp.logical_and(ok, test)
        return ok

    barrier = pltpu.get_barrier_semaphore()
    peers = n_rows - 1
    for side in SIDES:
        if side[0]:
            peers = peers + jnp.where(there(side), 1, 0)

            @pl.when(there(side))
            def _():
                pl.semaphore_signal(
                    barrier, inc=1, device_id=(gid, k + side[0], r + side[1]), device_id_type=MESH
                )
    for o in range(1, n_rows):
        pl.semaphore_signal(
            barrier, inc=1, device_id=(gid, k, lax.rem(r + o, n_rows)), device_id_type=MESH
        )

    def slot(s, count=1):
        at = s * LANE
        if not isinstance(at, int):
            at = pl.multiple_of(at, LANE)
        return pl.ds(at, count * LANE)

    blocks = {(0, -1): 0, (-1, -1): 1, (1, -1): 2, (0, 1): 3, (-1, 1): 4, (1, 1): 5}

    def exchange(index, shifts):
        made = []
        for i, side in enumerate(SIDES):
            dk, dr = side
            if dr == 0:
                src = shifts.at[1, :, slot(1 if dk < 0 else tile_cols)]
                dst = shifts.at[1, :, slot(tile_cols + 1 if dk < 0 else 0)]
            else:
                src = edge_out.at[index, pl.ds(0 if dr < 0 else PACK, PACK), :]
                dst = edge_in.at[index, pl.ds(PACK * blocks[(-dk, -dr)], PACK), :]
            made.append(
                pltpu.make_async_remote_copy(
                    src_ref=src,
                    dst_ref=dst,
                    send_sem=x_send.at[index, i],
                    recv_sem=x_recv.at[index, i],
                    device_id=(gid, k + dk, r + dr),
                    device_id_type=MESH,
                )
            )
        return made

    def opposite(i):
        return SIDES.index((-SIDES[i][0], -SIDES[i][1]))

    def send_edges(index, shifts):
        made = exchange(index, shifts)
        for i in (3, 2, 0, 1, 4, 5, 6, 7):
            @pl.when(there(SIDES[i]))
            def _():
                made[i].start()

    def await_edges(index, shifts):
        made = exchange(index, shifts)
        for i, side in enumerate(SIDES):
            @pl.when(there(side))
            def _():
                made[opposite(i)].wait_recv()

    def await_sent(index, shifts):
        made = exchange(index, shifts)
        for i, side in enumerate(SIDES):
            @pl.when(there(side))
            def _():
                made[i].wait_send()

    def clear_edges(index, shifts):
        for side in SIDES:
            dk, dr = side

            @pl.when(jnp.logical_not(there(side)))
            def _():
                if dr == 0:
                    shifts[1, :, slot(0 if dk < 0 else tile_cols + 1)] = jnp.zeros((C, LANE), BF)
                else:
                    edge_in[index, pl.ds(PACK * blocks[side], PACK), :] = jnp.zeros((PACK, tall), BF)

    def edge_picker(first, count):
        row = lax.broadcasted_iota(jnp.int32, (2 * PACK, count * LANE), 0)
        at = lax.broadcasted_iota(jnp.int32, (2 * PACK, count * LANE), 1)
        low = jnp.where(row < PACK, (row - 1 - first) * LANE, (row - PACK - first) * LANE - 1)
        real = jnp.where(row < PACK, row, row - PACK)
        hit = jnp.logical_and(at == low, jnp.logical_and(real > first, real <= first + count))
        return jnp.where(hit, 1.0, 0.0).astype(BF)

    def pad_rows(value):
        return jnp.concatenate([value, jnp.zeros((value.shape[0], tall - C), F32)], axis=1).astype(BF)

    def shift(shifts, s, halo, low, high):
        value = shifts[1, :, slot(s)].astype(F32)
        before = jnp.where(lane == 0, low(halo), pltpu.roll(value, 1, 1))
        after = jnp.where(lane == LANE - 1, high(halo), pltpu.roll(value, LANE - 1, 1))
        shifts[0, :, slot(s)] = before.astype(BF)
        shifts[2, :, slot(s)] = after.astype(BF)

    def shift_fixed(index, shifts, s, halo):
        if s == 0:
            at = PACK + tile_cols
        elif s == tile_cols + 1:
            at = 2 * PACK + 1
        else:
            at = s
        shift(
            shifts,
            s,
            halo,
            lambda h: h[:, at : at + 1],
            lambda h: h[:, at + 3 * PACK : at + 3 * PACK + 1],
        )

    def halo_of(ref):
        return ref[...].astype(F32).T[:C]

    def control_halo(start, count, outer):
        parts = []
        if count:
            parts.append(cedge_in[pl.ds(pl.multiple_of(PACK * start, PACK), PACK * count), :])
        if outer is not None:
            parts.append(cedge_in[pl.ds(pl.multiple_of(PACK * outer, PACK), PACK), :])
        parts = [part.astype(F32) for part in parts]
        have = sum(part.shape[0] for part in parts)
        parts.append(jnp.zeros((LANE - have, tall), F32))
        return jnp.concatenate(parts, axis=0).T[:C]

    def shift_control(s, at, halo):
        shift(shifts_c, s, halo, lambda h: h[:, at : at + 1], lambda h: h[:, at + 1 : at + 2])

    def shift_half(start, halo):
        for c in range(half_cols):
            at = PACK * (c // strip_cols) + 2 * (c % strip_cols)
            shift_control(start + c + 1, at, halo)

    def shift_outer(on_left, at, halo):
        value = jnp.where(on_left == 1, pltpu.roll(halo, LANE - 2 * (strip_cols - 1), 1), halo)
        shift_control((1 - on_left) * (tile_cols + 1), at, value)

    def pack_weights(i):
        weight_loads[i].wait()
        for t in range(9):
            packed[i, :, pl.ds(t * main, main)] = raw[i, t, :, :main]
        for t in range(0, 9, 2):
            here = raw[i, t, :, main:]
            at = 9 * main + t * rest
            if t < 8:
                here = jnp.concatenate([here, raw[i, t + 1, :, main:]], axis=1)
            packed[i, :, pl.ds(at, here.shape[1])] = here

    def convolve(i, shifts, runs):
        pieces, last = [], []
        for t in range(9):
            top = [shifts[t % 3, :main, slot(c + t // 3, n)] for c, n in runs]
            low = [shifts[t % 3, main:, slot(c + t // 3, n)] for c, n in runs]
            pieces.append(jnp.concatenate(top, axis=1) if len(top) > 1 else top[0])
            last.append(jnp.concatenate(low, axis=1) if len(low) > 1 else low[0])
        patch = jnp.concatenate(pieces + last, axis=0)
        total = jnp.dot(packed[i], patch, preferred_element_type=F32)
        count = sum(n for _, n in runs)
        return silu(total + jnp.concatenate([biases[i]] * count, axis=1))

    base_load.wait()
    for w in range(tile_cols):
        shifts_b[1, :, slot(w + 1)] = base[pl.ds(w, C, tile_cols), :].astype(BF)
    edge_out[0] = pad_rows(
        lax.dot_general(
            edge_picker(0, tile_cols),
            shifts_b[1, :, slot(1, tile_cols)],
            NT,
            preferred_element_type=F32,
        )
    )
    pl.semaphore_wait(barrier, peers)
    send_edges(0, shifts_b)

    def make_strip(q):
        for w in range(strip_cols):
            strips[q, :, w * LANE : (w + 1) * LANE] = flat[
                pl.ds(q * C * strip_cols + w, C, strip_cols), :
            ].astype(BF)

    def to_tile(q, w):
        return pltpu.make_async_remote_copy(
            src_ref=strips.at[q, :, slot(w)],
            dst_ref=shifts_c.at[1, :, slot(r * strip_cols + w + 1)],
            send_sem=in_send.at[q, w],
            recv_sem=in_recv.at[r, w],
            device_id=(gid, k, q),
            device_id_type=MESH,
        )

    def from_strip(q, w):
        return pltpu.make_async_remote_copy(
            src_ref=strips.at[q, :, slot(w)],
            dst_ref=shifts_c.at[1, :, slot(q * strip_cols + w + 1)],
            send_sem=in_send.at[q, w],
            recv_sem=in_recv.at[q, w],
            device_id=(gid, k, q),
            device_id_type=MESH,
        )

    def control_edges(q, to):
        return pltpu.make_async_remote_copy(
            src_ref=cedge_out.at[q],
            dst_ref=cedge_in.at[pl.ds(pl.multiple_of(PACK * (1 + to), PACK), PACK), :],
            send_sem=ce_send.at[q],
            recv_sem=ce_recv.at[to],
            device_id=(gid, k, q),
            device_id_type=MESH,
        )

    def forward(i):
        to_left = far_is_left if i else 1 - far_is_left
        step = 1 - 2 * to_left
        src_slot = 1 + (1 - to_left) * (tile_cols - 1)
        dst_slot = to_left * (tile_cols + 1)
        src_block = 1 + (1 - to_left) * (n_rows - 1)
        dst_block = to_left * (n_rows + 1)
        made = (
            pltpu.make_async_remote_copy(
                src_ref=shifts_c.at[1, :, slot(src_slot)],
                dst_ref=shifts_c.at[1, :, slot(dst_slot)],
                send_sem=fw_send.at[i, 0],
                recv_sem=fw_recv.at[i, 0],
                device_id=(gid, k + step, r),
                device_id_type=MESH,
            ),
            pltpu.make_async_remote_copy(
                src_ref=cedge_in.at[pl.ds(pl.multiple_of(PACK * src_block, PACK), PACK), :],
                dst_ref=cedge_in.at[pl.ds(pl.multiple_of(PACK * dst_block, PACK), PACK), :],
                send_sem=fw_send.at[i, 1],
                recv_sem=fw_recv.at[i, 1],
                device_id=(gid, k + step, r),
                device_id_type=MESH,
            ),
        )
        goes = jnp.where(to_left == 1, k > 0, k < n_cols - 1)
        comes = jnp.where(to_left == 1, k < n_cols - 1, k > 0)
        return made, goes, comes

    def forward_start(i):
        made, goes, _ = forward(i)

        @pl.when(goes)
        def _():
            for copy in made:
                copy.start()

    def forward_recv(i):
        made, _, comes = forward(i)

        @pl.when(comes)
        def _():
            for copy in made:
                copy.wait_recv()

    def forward_sent(i):
        made, goes, _ = forward(i)

        @pl.when(goes)
        def _():
            for copy in made:
                copy.wait_send()

    def to_strip(q, source):
        return pltpu.make_async_remote_copy(
            src_ref=bracket.at[q],
            dst_ref=arrived.at[source],
            send_sem=out_send.at[q],
            recv_sem=out_recv.at[source],
            device_id=(gid, k, q),
            device_id_type=MESH,
        )

    for copy in ctl_loads:
        copy.wait()
    for q in fars:
        make_strip(q)
    for w in range(strip_cols):
        to_tile(fars[0], w).start()
    for q in buddies:
        make_strip(q)
        for w in range(strip_cols):
            to_tile(q, w).start()
    make_strip(r)
    shifts_c[1, :, slot(r * strip_cols + 1, strip_cols)] = strips[r]

    row = lax.broadcasted_iota(jnp.int32, (2 * PACK, wide), 0)
    at = lax.broadcasted_iota(jnp.int32, (2 * PACK, wide), 1)
    real = jnp.where(row < PACK, row, row - PACK)
    w_of = lax.div(real, 2)
    want = jnp.where(row < PACK, w_of * LANE + LANE - 1, w_of * LANE)
    parity = jnp.where(row < PACK, 0, 1)
    hit = jnp.logical_and(at == want, jnp.logical_and(lax.rem(real, 2) == parity, w_of < strip_cols))
    picker = jnp.where(hit, 1.0, 0.0).astype(BF)
    found = [
        lax.dot_general(picker, strips[q], NT, preferred_element_type=F32) for q in range(n_rows)
    ]
    for q in range(n_rows):
        value = None
        if q > 0:
            value = found[q - 1][:PACK]
        if q < n_rows - 1:
            value = found[q + 1][PACK:] if value is None else value + found[q + 1][PACK:]
        cedge_out[q] = pad_rows(value)
    for q in buddies + fars:
        control_edges(q, r).start()
    cedge_in[pl.ds(pl.multiple_of(PACK * (1 + r), PACK), PACK), :] = cedge_out[r]
    for q in fars[1:-1]:
        for w in range(strip_cols):
            to_tile(q, w).start()
    if half > 1:
        to_tile(fars[-1], 0).start()

    for copy in row_loads:
        copy.wait()
    for i, ref in enumerate((row1, row2, row3)):
        line = jnp.concatenate([ref[...][None], jnp.zeros((1, tall - C), F32)], axis=1)
        biases[i] = jnp.broadcast_to(line, (LANE, tall)).T[:C]
    for index, shifts in enumerate((shifts_b, shifts_h)):
        clear_edges(index, shifts)

    @pl.when(k == 0)
    def _():
        shifts_c[1, :, slot(0)] = jnp.zeros((C, LANE), BF)
        cedge_in[pl.ds(0, PACK), :] = jnp.zeros((PACK, tall), BF)

    @pl.when(k == n_cols - 1)
    def _():
        shifts_c[1, :, slot(tile_cols + 1)] = jnp.zeros((C, LANE), BF)
        cedge_in[pl.ds(PACK * (n_rows + 1), PACK), :] = jnp.zeros((PACK, tall), BF)

    pack_weights(0)

    await_edges(0, shifts_b)
    halo = halo_of(edge_in.at[0])
    ready = 0
    edges = None
    for q in range(n_rows):
        while ready < (q + 1) * strip_cols + 2:
            shift_fixed(0, shifts_b, ready, halo)
            ready += 1
        value = convolve(0, shifts_b, [(q * strip_cols, strip_cols)]).astype(BF)
        shifts_h[1, :, slot(q * strip_cols + 1, strip_cols)] = value
        part = lax.dot_general(
            edge_picker(q * strip_cols, strip_cols), value, NT, preferred_element_type=F32
        )
        edges = part if edges is None else edges + part
    edge_out[1] = pad_rows(edges)
    send_edges(1, shifts_h)
    for w in range(1 if half > 1 else 0, strip_cols):
        if half > 1:
            to_tile(fars[-1], w).start()

    pack_weights(2)
    for q in buddies:
        for w in range(strip_cols):
            from_strip(q, w).wait_recv()
        control_edges(q, q).wait_recv()
    forward_start(0)
    shift_half(near_start, control_halo(1 + near_base, half, None))
    inner = []
    left = half_cols - 2
    while left > 0:
        take = min(left, strip_cols)
        inner.append([(near_start + half_cols - 1 - left, take)])
        left -= take
    for i, runs in enumerate(inner):
        inner_mid[i, :, : runs[0][1] * LANE] = convolve(2, shifts_c, runs)
    pack_weights(1)

    await_edges(1, shifts_h)
    halo = halo_of(edge_in.at[1])
    for s in range(tile_cols + 2):
        shift_fixed(1, shifts_h, s, halo)

    def second(start):
        own = jnp.concatenate(
            [base[pl.ds(start + w, C, tile_cols), :] for w in range(strip_cols)], axis=1
        )
        mid[:, slot(start, strip_cols)] = convolve(1, shifts_h, [(start, strip_cols)]) + own

    def columns(ref, runs):
        parts = [ref[:, slot(c, n)] for c, n in runs]
        return jnp.concatenate(parts, axis=1) if len(parts) > 1 else parts[0]

    def change_of(middle, runs):
        return middle + jnp.dot(
            tc_ref[...], columns(mid, runs).astype(BF), preferred_element_type=F32
        )

    def put_base(change, runs):
        control = columns(shifts_c.at[1], [(c + 1, n) for c, n in runs]).astype(F32)
        value = columns(mid, runs) + jnp.dot(
            tb_ref[...], (change + control).astype(BF), preferred_element_type=F32
        )
        done = 0
        for c, n in runs:
            for w in range(n):
                base_new[pl.ds(c + w, C, tile_cols), :] = value[:, done * LANE : (done + 1) * LANE]
                done += 1

    for q in fars:
        second(q * strip_cols)

    for copy in t_loads:
        copy.wait()
    for q in fars:
        for w in range(strip_cols):
            from_strip(q, w).wait_recv()
        control_edges(q, q).wait_recv()
    forward_start(1)
    forward_recv(0)
    halo = control_halo(1 + far_base, half, (1 - far_is_left) * (n_rows + 1))
    shift_half(far_start, halo)
    shift_outer(far_is_left, PACK * half, halo)
    for q in fars:
        runs = [(q * strip_cols, strip_cols)]
        change = change_of(convolve(2, shifts_c, runs), runs)
        bracket[q] = change.astype(BF)
        to_strip(q, r).start()
        put_base(change, runs)

    for i in range(half):
        second((near_base + i) * strip_cols)
    for i, runs in enumerate(inner):
        change = change_of(inner_mid[i, :, : runs[0][1] * LANE], runs)
        for w in range(runs[0][1]):
            col = half_cols - 1 - (half_cols - 2 - i * strip_cols) + w
            bracket[near_base + col // strip_cols, :, slot(col % strip_cols)] = change[
                :, w * LANE : (w + 1) * LANE
            ].astype(BF)
        put_base(change, runs)

    forward_recv(1)
    halo = control_halo(0, 0, far_is_left * (n_rows + 1))
    shift_outer(1 - far_is_left, 0, halo)
    runs = [(near_start, 1), (near_start + half_cols - 1, 1)]
    change = change_of(convolve(2, shifts_c, runs), runs)
    bracket[near_base, :, slot(0)] = change[:, :LANE].astype(BF)
    bracket[near_base + half - 1, :, slot(strip_cols - 1)] = change[:, LANE:].astype(BF)
    for q in buddies:
        to_strip(q, r).start()
    put_base(change, runs)
    arrived[r] = bracket[r]

    def finish(q):
        for w in range(strip_cols):
            where = pl.ds(q * C * strip_cols + w, C, strip_cols)
            flat[where, :] = flat[where, :] + arrived[q, :, slot(w)].astype(F32)

    finish(r)
    for q in buddies + fars:
        to_strip(q, q).wait_recv()
        finish(q)
    for index, shifts in enumerate((shifts_b, shifts_h)):
        await_sent(index, shifts)
    for i in range(2):
        forward_sent(i)
    for q in buddies + fars:
        for w in range(strip_cols):
            to_tile(q, w).wait_send()
        control_edges(q, r).wait_send()
        to_strip(q, r).wait_send()


def deliver(base_new, ctl, base_out, control_out, sem):
    n_rows = ctl.shape[0]
    copies = [pltpu.make_async_copy(base_new, base_out, sem.at[n_rows])]
    for q in range(n_rows):
        copies.append(
            pltpu.make_async_copy(
                ctl.at[q], control_out.at[:, :, pl.ds(q * LANE, LANE)], sem.at[q]
            )
        )
    for copy in copies:
        copy.start()
    for copy in copies:
        copy.wait()


def solution(mesh):
    n_cols, n_rows = mesh.shape["cols"], mesh.shape["rows"]

    def per_device(base, control, k1, k2, kc, b1, b2, bc, tc, tb):
        C, tile_cols, _ = base.shape
        strip_cols = control.shape[1]
        wide = strip_cols * LANE
        tall = -(-C // LANE) * LANE
        area = tile_cols * LANE
        half = n_rows // 2
        held = pltpu.VMEM((3, C, area + 2 * LANE), BF)
        inner = max(1, -(-(half * strip_cols - 2) // strip_cols))
        hbm = pl.BlockSpec(memory_space=pltpu.HBM)
        vmem = pl.BlockSpec(memory_space=pltpu.VMEM)
        base_new, ctl = pl.pallas_call(
            functools.partial(kernel, n_cols, n_rows),
            out_shape=(
                pltpu.VMEM((C * tile_cols, LANE), F32),
                pltpu.VMEM((n_rows, C, strip_cols, LANE), F32),
            ),
            in_specs=[hbm] * 10,
            out_specs=(vmem, vmem),
            scratch_shapes=[
                pltpu.VMEM((C * tile_cols, LANE), F32),
                pltpu.VMEM((3,) + k1.shape, BF),
                pltpu.VMEM((3, C, 9 * C), BF),
                held,
                held,
                held,
                pltpu.VMEM((C,), F32),
                pltpu.VMEM((C,), F32),
                pltpu.VMEM((C,), F32),
                pltpu.VMEM((3, C, LANE), F32),
                pltpu.VMEM((C, C), BF),
                pltpu.VMEM((C, C), BF),
                pltpu.VMEM((2, 2 * PACK, tall), BF),
                pltpu.VMEM((2, LANE, tall), BF),
                pltpu.VMEM((n_rows, PACK, tall), BF),
                pltpu.VMEM((LANE, tall), BF),
                pltpu.VMEM((n_rows, C, wide), BF),
                pltpu.VMEM((C, area), F32),
                pltpu.VMEM((inner, C, wide), F32),
                pltpu.VMEM((n_rows, C, wide), BF),
                pltpu.VMEM((n_rows, C, wide), BF),
                pltpu.SemaphoreType.DMA((9 + n_rows,)),
                pltpu.SemaphoreType.DMA((2, 8)),
                pltpu.SemaphoreType.DMA((2, 8)),
                pltpu.SemaphoreType.DMA((n_rows, strip_cols)),
                pltpu.SemaphoreType.DMA((n_rows, strip_cols)),
                pltpu.SemaphoreType.DMA((n_rows,)),
                pltpu.SemaphoreType.DMA((n_rows,)),
                pltpu.SemaphoreType.DMA((2, 2)),
                pltpu.SemaphoreType.DMA((2, 2)),
                pltpu.SemaphoreType.DMA((n_rows,)),
                pltpu.SemaphoreType.DMA((n_rows,)),
            ],
            compiler_params=pltpu.CompilerParams(
                collective_id=0, has_side_effects=True, vmem_limit_bytes=60 * 1024 * 1024
            ),
        )(base.reshape(C * tile_cols, LANE), control, k1, k2, kc, b1, b2, bc, tc, tb)
        base_out, control_out = pl.pallas_call(
            deliver,
            out_shape=(
                jax.ShapeDtypeStruct(base_new.shape, F32),
                jax.ShapeDtypeStruct(control.shape, F32),
            ),
            in_specs=[vmem] * 2,
            out_specs=(hbm, hbm),
            scratch_shapes=[pltpu.SemaphoreType.DMA((n_rows + 1,))],
            compiler_params=pltpu.CompilerParams(vmem_limit_bytes=1024 * 1024),
        )(base_new, ctl)
        return base_out.reshape(base.shape), control_out

    tiles = P(None, ("groups", "cols"), "rows")
    lines = P(None, ("groups", "cols", "rows"), None)
    return jax.shard_map(
        per_device,
        mesh=mesh,
        in_specs=(tiles, lines) + (P(),) * 8,
        out_specs=(tiles, lines),
        check_vma=False,
    )
```

```python
import functools

import jax
import jax.numpy as jnp
from jax import lax
from jax.experimental import pallas as pl
from jax.experimental.pallas import tpu as pltpu
from jax.sharding import PartitionSpec as P

MESH = pl.DeviceIdType.MESH
BF = jnp.bfloat16
F32 = jnp.float32
LANE = 128
PACK = 16
SIDES = ((-1, 0), (1, 0), (0, -1), (0, 1), (-1, -1), (1, -1), (-1, 1), (1, 1))
ROW_SIDES = ((0, 1), (0, -1))
WIDE_SIDES = tuple(side for side in SIDES if side[0])
NT = (((1,), (1,)), ((), ()))


def silu(v):
    return 0.5 * v * (1.0 + jnp.tanh(0.5 * v))


def kernel(
    n_cols,
    n_rows,
    base_hbm,
    control_hbm,
    k1_hbm,
    k2_hbm,
    kc_hbm,
    b1_hbm,
    b2_hbm,
    bc_hbm,
    tc_hbm,
    tb_hbm,
    base_new,
    ctl,
    base,
    raw,
    packed,
    shifts_b,
    shifts_h,
    shifts_c,
    row1,
    row2,
    row3,
    biases,
    tc_ref,
    tb_ref,
    edge_out,
    edge_in,
    cedge_out,
    cedge_in,
    strips,
    mid,
    inner_mid,
    far_change,
    bracket,
    arrived,
    load_sem,
    x_send,
    x_recv,
    in_send,
    in_recv,
    ce_send,
    ce_recv,
    fw_send,
    fw_recv,
    out_send,
    out_recv,
):
    C = tc_ref.shape[0]
    tile_cols = base.shape[0] // C
    strip_cols = ctl.shape[2]
    wide = strip_cols * LANE
    main = C - C % LANE
    rest = C - main
    tall = edge_out.shape[2]
    half = n_rows // 2
    half_cols = half * strip_cols
    assert n_rows == 2 * half and half_cols == strip_cols + 2 and 2 * half_cols == tile_cols
    gid = lax.axis_index("groups")
    k = lax.axis_index("cols")
    r = lax.axis_index("rows")
    lane = lax.broadcasted_iota(jnp.int32, (C, LANE), 1)
    flat = ctl.reshape(n_rows * C * strip_cols, LANE)

    near_base = half * lax.div(r, half)
    far_base = half - near_base
    far_is_left = lax.div(r, half)
    near_start = near_base * strip_cols
    far_start = far_base * strip_cols
    buddies = [near_base + lax.rem(r - near_base + o, half) for o in range(1, half)]
    fars = [far_base + j for j in range(half)]
    inward = [far_base + j + far_is_left * (half - 1 - 2 * j) for j in range(half)]

    def load(i, src, dst):
        copy = pltpu.make_async_copy(src, dst, load_sem.at[i])
        copy.start()
        return copy

    base_load = load(0, base_hbm, base)
    ctl_loads = [
        load(1 + q, control_hbm.at[:, :, pl.ds(q * LANE, LANE)], ctl.at[q]) for q in range(n_rows)
    ]
    more = 1 + n_rows
    weight_loads = [load(more, k1_hbm, raw.at[0])]
    row_loads = [
        load(more + 3 + i, src, dst)
        for i, (src, dst) in enumerate(((b1_hbm, row1), (b2_hbm, row2), (bc_hbm, row3)))
    ]
    weight_loads.append(load(more + 2, kc_hbm, raw.at[2]))
    weight_loads.insert(1, load(more + 1, k2_hbm, raw.at[1]))
    t_loads = [load(more + 6, tc_hbm, tc_ref), load(more + 7, tb_hbm, tb_ref)]

    def there(side):
        dk, dr = side
        ok = None
        for at, step, count in ((k, dk, n_cols), (r, dr, n_rows)):
            if step:
                test = (at > 0) if step < 0 else (at < count - 1)
                ok = test if ok is None else jnp.logical_and(ok, test)
        return ok

    barrier = pltpu.get_barrier_semaphore()
    peers = n_rows - 1
    for side in SIDES:
        if side[0]:
            peers = peers + jnp.where(there(side), 1, 0)

            @pl.when(there(side))
            def _():
                pl.semaphore_signal(
                    barrier, inc=1, device_id=(gid, k + side[0], r + side[1]), device_id_type=MESH
                )
    for o in range(1, n_rows):
        pl.semaphore_signal(
            barrier, inc=1, device_id=(gid, k, lax.rem(r + o, n_rows)), device_id_type=MESH
        )

    def slot(s, count=1):
        at = s * LANE
        if not isinstance(at, int):
            at = pl.multiple_of(at, LANE)
        return pl.ds(at, count * LANE)

    blocks = {(0, -1): 0, (0, 1): 1, (-1, -1): 2, (1, -1): 3, (-1, 1): 4, (1, 1): 5}

    def exchange(index, shifts, which):
        made = []
        for side in which:
            i = SIDES.index(side)
            dk, dr = side
            if dr == 0:
                src = shifts.at[1, :, slot(1 if dk < 0 else tile_cols)]
                dst = shifts.at[1, :, slot(tile_cols + 1 if dk < 0 else 0)]
            else:
                src = edge_out.at[index, pl.ds(0 if dr < 0 else PACK, PACK), :]
                dst = edge_in.at[index, pl.ds(PACK * blocks[(-dk, -dr)], PACK), :]
            made.append(
                pltpu.make_async_remote_copy(
                    src_ref=src,
                    dst_ref=dst,
                    send_sem=x_send.at[index, i],
                    recv_sem=x_recv.at[index, i],
                    device_id=(gid, k + dk, r + dr),
                    device_id_type=MESH,
                )
            )
        return made

    def send_edges(index, shifts, which):
        for side, copy in zip(which, exchange(index, shifts, which)):
            @pl.when(there(side))
            def _():
                copy.start()

    def await_edges(index, shifts, which):
        facing = [(-side[0], -side[1]) for side in which]
        for side, copy in zip(which, exchange(index, shifts, facing)):
            @pl.when(there(side))
            def _():
                copy.wait_recv()

    def await_sent(index, shifts, which):
        for side, copy in zip(which, exchange(index, shifts, which)):
            @pl.when(there(side))
            def _():
                copy.wait_send()

    def clear_edges(index, shifts, which):
        for side in which:
            dk, dr = side

            @pl.when(jnp.logical_not(there(side)))
            def _():
                if dr == 0:
                    shifts[1, :, slot(0 if dk < 0 else tile_cols + 1)] = jnp.zeros((C, LANE), BF)
                else:
                    edge_in[index, pl.ds(PACK * blocks[side], PACK), :] = jnp.zeros((PACK, tall), BF)

    def edge_picker(first, count):
        row = lax.broadcasted_iota(jnp.int32, (2 * PACK, count * LANE), 0)
        at = lax.broadcasted_iota(jnp.int32, (2 * PACK, count * LANE), 1)
        low = jnp.where(row < PACK, (row - 1 - first) * LANE, (row - PACK - first) * LANE - 1)
        real = jnp.where(row < PACK, row, row - PACK)
        hit = jnp.logical_and(at == low, jnp.logical_and(real > first, real <= first + count))
        return jnp.where(hit, 1.0, 0.0).astype(BF)

    def pad_rows(value):
        return jnp.concatenate([value, jnp.zeros((value.shape[0], tall - C), F32)], axis=1).astype(BF)

    def move(value, by):
        by = by % LANE
        return pltpu.roll(value, by, 1) if by else value

    def shift(shifts, s, halo, low, high):
        value = shifts[1, :, slot(s)]
        shifts[0, :, slot(s)] = jnp.where(lane == 0, move(halo, -low), move(value, 1))
        shifts[2, :, slot(s)] = jnp.where(
            lane == LANE - 1, move(halo, LANE - 1 - high), move(value, -1)
        )

    def turn(parts):
        have = sum(part.shape[0] for part in parts)
        parts = [part.astype(F32) for part in parts] + [jnp.zeros((LANE - have, tall), F32)]
        return jnp.concatenate(parts, axis=0).T[:C].astype(BF)

    def tile_halo(index, count):
        return turn([edge_in[index, : PACK * count, :]])

    def shift_inner(shifts, s, halo):
        shift(shifts, s, halo, s, PACK + s)

    def shift_ends(shifts, halo):
        shift(shifts, 0, halo, 2 * PACK + tile_cols, 4 * PACK + tile_cols)
        shift(shifts, tile_cols + 1, halo, 3 * PACK + 1, 5 * PACK + 1)

    def control_halo(start, count, outer):
        parts = []
        if count:
            parts.append(cedge_in[pl.ds(pl.multiple_of(PACK * start, PACK), PACK * count), :])
        if outer is not None:
            parts.append(cedge_in[pl.ds(pl.multiple_of(PACK * outer, PACK), PACK), :])
        return turn(parts)

    def shift_control(s, at, halo):
        shift(shifts_c, s, halo, at, at + 1)

    def shift_half(start, halo):
        for c in range(half_cols):
            at = PACK * (c // strip_cols) + 2 * (c % strip_cols)
            shift_control(start + c + 1, at, halo)

    def shift_outer(on_left, at, halo):
        value = jnp.where(on_left == 1, move(halo, -2 * (strip_cols - 1)), halo)
        shift_control((1 - on_left) * (tile_cols + 1), at, value)

    def pack_weights(i):
        weight_loads[i].wait()
        for t in range(9):
            packed[i, :, pl.ds(t * main, main)] = raw[i, t, :, :main]
        for t in range(0, 9, 2):
            here = raw[i, t, :, main:]
            at = 9 * main + t * rest
            if t < 8:
                here = jnp.concatenate([here, raw[i, t + 1, :, main:]], axis=1)
            packed[i, :, pl.ds(at, here.shape[1])] = here

    def product(ref, right):
        middle = C // 2 // PACK * PACK
        return jnp.concatenate(
            [
                jnp.dot(ref[:middle, :], right, preferred_element_type=F32),
                jnp.dot(ref[middle:, :], right, preferred_element_type=F32),
            ],
            axis=0,
        )

    def convolve(i, shifts, runs):
        pieces, last = [], []
        for t in range(9):
            top = [shifts[t % 3, :main, slot(c + t // 3, n)] for c, n in runs]
            low = [shifts[t % 3, main:, slot(c + t // 3, n)] for c, n in runs]
            pieces.append(jnp.concatenate(top, axis=1) if len(top) > 1 else top[0])
            last.append(jnp.concatenate(low, axis=1) if len(low) > 1 else low[0])
        patch = jnp.concatenate(pieces + last, axis=0)
        total = product(packed.at[i], patch)
        count = sum(n for _, n in runs)
        return silu(total + jnp.concatenate([biases[i]] * count, axis=1))

    base_load.wait()
    for w in range(tile_cols):
        shifts_b[1, :, slot(w + 1)] = base[pl.ds(w, C, tile_cols), :].astype(BF)
    edge_out[0] = pad_rows(
        lax.dot_general(
            edge_picker(0, tile_cols),
            shifts_b[1, :, slot(1, tile_cols)],
            NT,
            preferred_element_type=F32,
        )
    )
    pl.semaphore_wait(barrier, peers)
    send_edges(0, shifts_b, ROW_SIDES + WIDE_SIDES)

    def make_strip(q):
        for w in range(strip_cols):
            strips[q, :, w * LANE : (w + 1) * LANE] = flat[
                pl.ds(q * C * strip_cols + w, C, strip_cols), :
            ].astype(BF)

    def to_tile(q, w):
        return pltpu.make_async_remote_copy(
            src_ref=strips.at[q, :, slot(w)],
            dst_ref=shifts_c.at[1, :, slot(r * strip_cols + w + 1)],
            send_sem=in_send.at[q, w],
            recv_sem=in_recv.at[r, w],
            device_id=(gid, k, q),
            device_id_type=MESH,
        )

    def from_strip(q, w):
        return pltpu.make_async_remote_copy(
            src_ref=strips.at[q, :, slot(w)],
            dst_ref=shifts_c.at[1, :, slot(q * strip_cols + w + 1)],
            send_sem=in_send.at[q, w],
            recv_sem=in_recv.at[q, w],
            device_id=(gid, k, q),
            device_id_type=MESH,
        )

    def control_edges(q, to):
        return pltpu.make_async_remote_copy(
            src_ref=cedge_out.at[q],
            dst_ref=cedge_in.at[pl.ds(pl.multiple_of(PACK * (1 + to), PACK), PACK), :],
            send_sem=ce_send.at[q],
            recv_sem=ce_recv.at[to],
            device_id=(gid, k, q),
            device_id_type=MESH,
        )

    def forward(i):
        to_left = far_is_left if i else 1 - far_is_left
        step = 1 - 2 * to_left
        src_slot = 1 + (1 - to_left) * (tile_cols - 1)
        dst_slot = to_left * (tile_cols + 1)
        src_block = 1 + (1 - to_left) * (n_rows - 1)
        dst_block = to_left * (n_rows + 1)
        made = (
            pltpu.make_async_remote_copy(
                src_ref=shifts_c.at[1, :, slot(src_slot)],
                dst_ref=shifts_c.at[1, :, slot(dst_slot)],
                send_sem=fw_send.at[i, 0],
                recv_sem=fw_recv.at[i, 0],
                device_id=(gid, k + step, r),
                device_id_type=MESH,
            ),
            pltpu.make_async_remote_copy(
                src_ref=cedge_in.at[pl.ds(pl.multiple_of(PACK * src_block, PACK), PACK), :],
                dst_ref=cedge_in.at[pl.ds(pl.multiple_of(PACK * dst_block, PACK), PACK), :],
                send_sem=fw_send.at[i, 1],
                recv_sem=fw_recv.at[i, 1],
                device_id=(gid, k + step, r),
                device_id_type=MESH,
            ),
        )
        goes = jnp.where(to_left == 1, k > 0, k < n_cols - 1)
        comes = jnp.where(to_left == 1, k < n_cols - 1, k > 0)
        return made, goes, comes

    def forward_start(i):
        made, goes, _ = forward(i)

        @pl.when(goes)
        def _():
            for copy in made:
                copy.start()

    def forward_recv(i):
        made, _, comes = forward(i)

        @pl.when(comes)
        def _():
            for copy in made:
                copy.wait_recv()

    def forward_sent(i):
        made, goes, _ = forward(i)

        @pl.when(goes)
        def _():
            for copy in made:
                copy.wait_send()

    def to_strip(q, source):
        return pltpu.make_async_remote_copy(
            src_ref=bracket.at[q],
            dst_ref=arrived.at[source],
            send_sem=out_send.at[q],
            recv_sem=out_recv.at[source],
            device_id=(gid, k, q),
            device_id_type=MESH,
        )

    for copy in ctl_loads:
        copy.wait()
    for q in fars:
        make_strip(q)
    for w in range(strip_cols):
        to_tile(fars[0], w).start()
    for q in buddies:
        make_strip(q)
        for w in range(strip_cols):
            to_tile(q, w).start()
    make_strip(r)
    shifts_c[1, :, slot(r * strip_cols + 1, strip_cols)] = strips[r]

    row = lax.broadcasted_iota(jnp.int32, (2 * PACK, wide), 0)
    at = lax.broadcasted_iota(jnp.int32, (2 * PACK, wide), 1)
    real = jnp.where(row < PACK, row, row - PACK)
    w_of = lax.div(real, 2)
    want = jnp.where(row < PACK, w_of * LANE + LANE - 1, w_of * LANE)
    parity = jnp.where(row < PACK, 0, 1)
    hit = jnp.logical_and(at == want, jnp.logical_and(lax.rem(real, 2) == parity, w_of < strip_cols))
    picker = jnp.where(hit, 1.0, 0.0).astype(BF)
    found = [
        lax.dot_general(picker, strips[q], NT, preferred_element_type=F32) for q in range(n_rows)
    ]
    for q in range(n_rows):
        value = None
        if q > 0:
            value = found[q - 1][:PACK]
        if q < n_rows - 1:
            value = found[q + 1][PACK:] if value is None else value + found[q + 1][PACK:]
        cedge_out[q] = pad_rows(value)
    for q in buddies + fars:
        control_edges(q, r).start()
    cedge_in[pl.ds(pl.multiple_of(PACK * (1 + r), PACK), PACK), :] = cedge_out[r]
    for q in fars[1:-1]:
        for w in range(strip_cols):
            to_tile(q, w).start()
    if half > 1:
        to_tile(fars[-1], 0).start()

    for copy in row_loads:
        copy.wait()
    for i, ref in enumerate((row1, row2, row3)):
        line = jnp.concatenate([ref[...][None], jnp.zeros((1, tall - C), F32)], axis=1)
        biases[i] = jnp.broadcast_to(line, (LANE, tall)).T[:C]
    clear_edges(0, shifts_b, ROW_SIDES + WIDE_SIDES)
    clear_edges(1, shifts_h, ROW_SIDES)
    clear_edges(2, shifts_h, ROW_SIDES + WIDE_SIDES)

    @pl.when(k == 0)
    def _():
        shifts_c[1, :, slot(0)] = jnp.zeros((C, LANE), BF)
        cedge_in[pl.ds(0, PACK), :] = jnp.zeros((PACK, tall), BF)

    @pl.when(k == n_cols - 1)
    def _():
        shifts_c[1, :, slot(tile_cols + 1)] = jnp.zeros((C, LANE), BF)
        cedge_in[pl.ds(PACK * (n_rows + 1), PACK), :] = jnp.zeros((PACK, tall), BF)

    pack_weights(0)

    def hidden(runs):
        value = convolve(0, shifts_b, runs).astype(BF)
        total, done = None, 0
        for c, n in runs:
            here = value[:, done * LANE : (done + n) * LANE]
            shifts_h[1, :, slot(c + 1, n)] = here
            part = lax.dot_general(edge_picker(c, n), here, NT, preferred_element_type=F32)
            total = part if total is None else total + part
            done += n
        return total

    await_edges(0, shifts_b, ROW_SIDES)
    halo = tile_halo(0, 2)
    ready, edges, c = 1, None, 1
    while c < tile_cols - 1:
        take = min(strip_cols, tile_cols - 1 - c)
        while ready < c + take + 2:
            shift_inner(shifts_b, ready, halo)
            ready += 1
        part = hidden([(c, take)])
        edges = part if edges is None else edges + part
        c += take
    edge_out[1] = pad_rows(edges)
    send_edges(1, shifts_h, ROW_SIDES)
    if half > 1:
        for w in range(1, strip_cols):
            to_tile(fars[-1], w).start()

    await_edges(0, shifts_b, WIDE_SIDES)
    shift_ends(shifts_b, tile_halo(0, 6))
    edge_out[2] = pad_rows(hidden([(0, 1), (tile_cols - 1, 1)]))
    send_edges(2, shifts_h, ROW_SIDES + WIDE_SIDES)

    pack_weights(2)
    for q in buddies:
        for w in range(strip_cols):
            from_strip(q, w).wait_recv()
        control_edges(q, q).wait_recv()
    forward_start(0)
    shift_half(near_start, control_halo(1 + near_base, half, None))
    inner = []
    left = half_cols - 2
    while left > 0:
        take = min(left, strip_cols)
        inner.append([(near_start + half_cols - 1 - left, take)])
        left -= take
    for i, runs in enumerate(inner):
        inner_mid[i, :, : runs[0][1] * LANE] = convolve(2, shifts_c, runs)
    pack_weights(1)

    await_edges(1, shifts_h, ROW_SIDES)
    halo = tile_halo(1, 2)
    inner_start = inward[0] * strip_cols
    rolled = pltpu.roll(halo, lax.rem(LANE - inner_start, LANE), 1)
    for i in range(strip_cols + 2):
        shift(shifts_h, inner_start + i, rolled, i, PACK + i)

    def second(start):
        own = jnp.concatenate(
            [base[pl.ds(start + w, C, tile_cols), :] for w in range(strip_cols)], axis=1
        )
        mid[:, slot(start, strip_cols)] = convolve(1, shifts_h, [(start, strip_cols)]) + own

    def columns(ref, runs):
        parts = [ref[:, slot(c, n)] for c, n in runs]
        return jnp.concatenate(parts, axis=1) if len(parts) > 1 else parts[0]

    def change_of(middle, runs):
        return middle + product(tc_ref, columns(mid, runs).astype(BF))

    def put_base(change, runs):
        control = columns(shifts_c.at[1], [(c + 1, n) for c, n in runs]).astype(F32)
        value = columns(mid, runs) + product(tb_ref, (change + control).astype(BF))
        done = 0
        for c, n in runs:
            for w in range(n):
                base_new[pl.ds(c + w, C, tile_cols), :] = value[:, done * LANE : (done + 1) * LANE]
                done += 1

    second(inner_start)

    for copy in t_loads:
        copy.wait()
    for q in fars:
        for w in range(strip_cols):
            from_strip(q, w).wait_recv()
        control_edges(q, q).wait_recv()
    forward_start(1)
    shift_half(far_start, control_halo(1 + far_base, half, None))

    def far_part(j):
        q = inward[j]
        runs = [(q * strip_cols, strip_cols)]
        change = change_of(convolve(2, shifts_c, runs), runs)
        bracket[q] = change.astype(BF)
        to_strip(q, r).start()
        far_change[j] = change

    far_part(0)

    await_edges(2, shifts_h, ROW_SIDES + WIDE_SIDES)
    halo_inner = halo
    halo = tile_halo(2, 6)
    rest_start = far_is_left * (strip_cols + 2)
    rolled = pltpu.roll(halo_inner, lax.rem(LANE - 2 - rest_start, LANE), 1)
    for i in range(tile_cols - 2 - strip_cols - 2):
        shift(shifts_h, 2 + rest_start + i, rolled, i, PACK + i)
    shift_inner(shifts_h, 1, halo)
    shift_inner(shifts_h, tile_cols, halo)
    shift_ends(shifts_h, halo)
    for j in range(1, half):
        second(inward[j] * strip_cols)
    forward_recv(0)
    shift_outer(far_is_left, 0, control_halo(0, 0, (1 - far_is_left) * (n_rows + 1)))
    for j in range(1, half):
        far_part(j)
    for j in range(half):
        put_base(far_change[j], [(inward[j] * strip_cols, strip_cols)])

    for i in range(half):
        second((near_base + i) * strip_cols)
    for i, runs in enumerate(inner):
        change = change_of(inner_mid[i, :, : runs[0][1] * LANE], runs)
        for w in range(runs[0][1]):
            col = half_cols - 1 - (half_cols - 2 - i * strip_cols) + w
            bracket[near_base + col // strip_cols, :, slot(col % strip_cols)] = change[
                :, w * LANE : (w + 1) * LANE
            ].astype(BF)
        put_base(change, runs)

    forward_recv(1)
    halo = control_halo(0, 0, far_is_left * (n_rows + 1))
    shift_outer(1 - far_is_left, 0, halo)
    runs = [(near_start, 1), (near_start + half_cols - 1, 1)]
    change = change_of(convolve(2, shifts_c, runs), runs)
    bracket[near_base, :, slot(0)] = change[:, :LANE].astype(BF)
    bracket[near_base + half - 1, :, slot(strip_cols - 1)] = change[:, LANE:].astype(BF)
    for q in buddies:
        to_strip(q, r).start()
    put_base(change, runs)
    arrived[r] = bracket[r]

    def finish(q):
        for w in range(strip_cols):
            where = pl.ds(q * C * strip_cols + w, C, strip_cols)
            flat[where, :] = flat[where, :] + arrived[q, :, slot(w)].astype(F32)

    finish(r)
    for q in buddies + fars:
        to_strip(q, q).wait_recv()
        finish(q)
    await_sent(0, shifts_b, ROW_SIDES + WIDE_SIDES)
    await_sent(1, shifts_h, ROW_SIDES)
    await_sent(2, shifts_h, ROW_SIDES + WIDE_SIDES)
    for i in range(2):
        forward_sent(i)
    for q in buddies + fars:
        for w in range(strip_cols):
            to_tile(q, w).wait_send()
        control_edges(q, r).wait_send()
        to_strip(q, r).wait_send()


def deliver(base_new, ctl, base_out, control_out, sem):
    n_rows = ctl.shape[0]
    copies = [pltpu.make_async_copy(base_new, base_out, sem.at[n_rows])]
    for q in range(n_rows):
        copies.append(
            pltpu.make_async_copy(
                ctl.at[q], control_out.at[:, :, pl.ds(q * LANE, LANE)], sem.at[q]
            )
        )
    for copy in copies:
        copy.start()
    for copy in copies:
        copy.wait()


def solution(mesh):
    n_cols, n_rows = mesh.shape["cols"], mesh.shape["rows"]

    def per_device(base, control, k1, k2, kc, b1, b2, bc, tc, tb):
        C, tile_cols, _ = base.shape
        strip_cols = control.shape[1]
        wide = strip_cols * LANE
        tall = -(-C // LANE) * LANE
        area = tile_cols * LANE
        half = n_rows // 2
        held = pltpu.VMEM((3, C, area + 2 * LANE), BF)
        inner = max(1, -(-(half * strip_cols - 2) // strip_cols))
        hbm = pl.BlockSpec(memory_space=pltpu.HBM)
        vmem = pl.BlockSpec(memory_space=pltpu.VMEM)
        base_new, ctl = pl.pallas_call(
            functools.partial(kernel, n_cols, n_rows),
            out_shape=(
                pltpu.VMEM((C * tile_cols, LANE), F32),
                pltpu.VMEM((n_rows, C, strip_cols, LANE), F32),
            ),
            in_specs=[hbm] * 10,
            out_specs=(vmem, vmem),
            scratch_shapes=[
                pltpu.VMEM((C * tile_cols, LANE), F32),
                pltpu.VMEM((3,) + k1.shape, BF),
                pltpu.VMEM((3, C, 9 * C), BF),
                held,
                held,
                held,
                pltpu.VMEM((C,), F32),
                pltpu.VMEM((C,), F32),
                pltpu.VMEM((C,), F32),
                pltpu.VMEM((3, C, LANE), F32),
                pltpu.VMEM((C, C), BF),
                pltpu.VMEM((C, C), BF),
                pltpu.VMEM((3, 2 * PACK, tall), BF),
                pltpu.VMEM((3, LANE, tall), BF),
                pltpu.VMEM((n_rows, PACK, tall), BF),
                pltpu.VMEM((LANE, tall), BF),
                pltpu.VMEM((n_rows, C, wide), BF),
                pltpu.VMEM((C, area), F32),
                pltpu.VMEM((inner, C, wide), F32),
                pltpu.VMEM((half, C, wide), F32),
                pltpu.VMEM((n_rows, C, wide), BF),
                pltpu.VMEM((n_rows, C, wide), BF),
                pltpu.SemaphoreType.DMA((9 + n_rows,)),
                pltpu.SemaphoreType.DMA((3, 8)),
                pltpu.SemaphoreType.DMA((3, 8)),
                pltpu.SemaphoreType.DMA((n_rows, strip_cols)),
                pltpu.SemaphoreType.DMA((n_rows, strip_cols)),
                pltpu.SemaphoreType.DMA((n_rows,)),
                pltpu.SemaphoreType.DMA((n_rows,)),
                pltpu.SemaphoreType.DMA((2, 2)),
                pltpu.SemaphoreType.DMA((2, 2)),
                pltpu.SemaphoreType.DMA((n_rows,)),
                pltpu.SemaphoreType.DMA((n_rows,)),
            ],
            compiler_params=pltpu.CompilerParams(
                collective_id=0, has_side_effects=True, vmem_limit_bytes=60 * 1024 * 1024
            ),
        )(base.reshape(C * tile_cols, LANE), control, k1, k2, kc, b1, b2, bc, tc, tb)
        base_out, control_out = pl.pallas_call(
            deliver,
            out_shape=(
                jax.ShapeDtypeStruct(base_new.shape, F32),
                jax.ShapeDtypeStruct(control.shape, F32),
            ),
            in_specs=[vmem] * 2,
            out_specs=(hbm, hbm),
            scratch_shapes=[pltpu.SemaphoreType.DMA((n_rows + 1,))],
            compiler_params=pltpu.CompilerParams(vmem_limit_bytes=1024 * 1024),
        )(base_new, ctl)
        return base_out.reshape(base.shape), control_out

    tiles = P(None, ("groups", "cols"), "rows")
    lines = P(None, ("groups", "cols", "rows"), None)
    return jax.shard_map(
        per_device,
        mesh=mesh,
        in_specs=(tiles, lines) + (P(),) * 8,
        out_specs=(tiles, lines),
        check_vma=False,
    )
```

```python
import functools

import jax
import jax.numpy as jnp
from jax import lax
from jax.experimental import pallas as pl
from jax.experimental.pallas import tpu as pltpu
from jax.sharding import PartitionSpec as P

MESH = pl.DeviceIdType.MESH
BF = jnp.bfloat16
F32 = jnp.float32
LANE = 128
PACK = 16
SIDES = ((-1, 0), (1, 0), (0, -1), (0, 1), (-1, -1), (1, -1), (-1, 1), (1, 1))
ROW_SIDES = ((0, 1), (0, -1))
WIDE_SIDES = tuple(side for side in SIDES if side[0])
TAPS = (1, 4, 7, 0, 3, 6, 2, 5, 8)
NT = (((1,), (1,)), ((), ()))


def silu(v):
    return 0.5 * v * (1.0 + jnp.tanh(0.5 * v))


def kernel(
    n_cols,
    n_rows,
    base_hbm,
    control_hbm,
    k1_hbm,
    k2_hbm,
    kc_hbm,
    b1_hbm,
    b2_hbm,
    bc_hbm,
    tc_hbm,
    tb_hbm,
    base_new,
    ctl,
    base,
    raw,
    packed,
    b_low,
    b_mid,
    b_high,
    h_low,
    h_mid,
    h_high,
    c_low,
    c_mid,
    c_high,
    row1,
    row2,
    row3,
    biases,
    tc_ref,
    tb_ref,
    edge_out,
    edge_in,
    cedge_out,
    cedge_in,
    strips,
    mid,
    inner_mid,
    far_change,
    bracket,
    arrived,
    load_sem,
    x_send,
    x_recv,
    in_send,
    in_recv,
    ce_send,
    ce_recv,
    fw_send,
    fw_recv,
    out_send,
    out_recv,
):
    C = tc_ref.shape[0]
    tile_cols = base.shape[0] // C
    strip_cols = ctl.shape[2]
    wide = strip_cols * LANE
    main = C - C % LANE
    rest = C - main
    tall = edge_out.shape[2]
    half = n_rows // 2
    half_cols = half * strip_cols
    middle = C // 2 // PACK * PACK
    assert n_rows == 2 * half and half_cols == strip_cols + 2 and 2 * half_cols == tile_cols
    gid = lax.axis_index("groups")
    k = lax.axis_index("cols")
    r = lax.axis_index("rows")
    lane = lax.broadcasted_iota(jnp.int32, (C, LANE), 1)
    flat = ctl.reshape(n_rows * C * strip_cols, LANE)

    shifts_b = (b_low, b_mid, b_high)
    shifts_h = (h_low, h_mid, h_high)
    shifts_c = (c_low, c_mid, c_high)
    near_base = half * lax.div(r, half)
    far_base = half - near_base
    far_is_left = lax.div(r, half)
    near_start = near_base * strip_cols
    far_start = far_base * strip_cols
    buddies = [near_base + lax.rem(r - near_base + o, half) for o in range(1, half)]
    fars = [far_base + j for j in range(half)]
    inward = [far_base + j + far_is_left * (half - 1 - 2 * j) for j in range(half)]

    def load(i, src, dst):
        copy = pltpu.make_async_copy(src, dst, load_sem.at[i])
        copy.start()
        return copy

    base_load = load(0, base_hbm, base)
    ctl_loads = [
        load(1 + q, control_hbm.at[:, :, pl.ds(q * LANE, LANE)], ctl.at[q]) for q in range(n_rows)
    ]
    more = 1 + n_rows
    weight_loads = [load(more, k1_hbm, raw.at[0])]
    row_loads = [
        load(more + 3 + i, src, dst)
        for i, (src, dst) in enumerate(((b1_hbm, row1), (b2_hbm, row2), (bc_hbm, row3)))
    ]
    weight_loads.append(load(more + 2, kc_hbm, raw.at[2]))
    weight_loads.insert(1, load(more + 1, k2_hbm, raw.at[1]))
    t_loads = [load(more + 6, tc_hbm, tc_ref), load(more + 7, tb_hbm, tb_ref)]

    def there(side):
        dk, dr = side
        ok = None
        for at, step, count in ((k, dk, n_cols), (r, dr, n_rows)):
            if step:
                test = (at > 0) if step < 0 else (at < count - 1)
                ok = test if ok is None else jnp.logical_and(ok, test)
        return ok

    barrier = pltpu.get_barrier_semaphore()
    peers = n_rows - 1
    for side in SIDES:
        if side[0]:
            peers = peers + jnp.where(there(side), 1, 0)

            @pl.when(there(side))
            def _():
                pl.semaphore_signal(
                    barrier, inc=1, device_id=(gid, k + side[0], r + side[1]), device_id_type=MESH
                )
    for o in range(1, n_rows):
        pl.semaphore_signal(
            barrier, inc=1, device_id=(gid, k, lax.rem(r + o, n_rows)), device_id_type=MESH
        )

    def slot(s, count=1):
        at = s * LANE
        if not isinstance(at, int):
            at = pl.multiple_of(at, LANE)
        return pl.ds(at, count * LANE)

    blocks = {(0, -1): 0, (0, 1): 1, (-1, -1): 2, (1, -1): 3, (-1, 1): 4, (1, 1): 5}

    def exchange(index, shifts, which):
        made = []
        for side in which:
            i = SIDES.index(side)
            dk, dr = side
            if dr == 0:
                src = shifts[1].at[:, slot(1 if dk < 0 else tile_cols)]
                dst = shifts[1].at[:, slot(tile_cols + 1 if dk < 0 else 0)]
            else:
                src = edge_out.at[index, pl.ds(0 if dr < 0 else PACK, PACK), :]
                dst = edge_in.at[index, pl.ds(PACK * blocks[(-dk, -dr)], PACK), :]
            made.append(
                pltpu.make_async_remote_copy(
                    src_ref=src,
                    dst_ref=dst,
                    send_sem=x_send.at[index, i],
                    recv_sem=x_recv.at[index, i],
                    device_id=(gid, k + dk, r + dr),
                    device_id_type=MESH,
                )
            )
        return made

    def send_edges(index, shifts, which):
        for side, copy in zip(which, exchange(index, shifts, which)):
            @pl.when(there(side))
            def _():
                copy.start()

    def await_edges(index, shifts, which):
        facing = [(-side[0], -side[1]) for side in which]
        for side, copy in zip(which, exchange(index, shifts, facing)):
            @pl.when(there(side))
            def _():
                copy.wait_recv()

    def await_sent(index, shifts, which):
        for side, copy in zip(which, exchange(index, shifts, which)):
            @pl.when(there(side))
            def _():
                copy.wait_send()

    def clear_edges(index, shifts, which):
        for side in which:
            dk, dr = side

            @pl.when(jnp.logical_not(there(side)))
            def _():
                if dr == 0:
                    shifts[1][:, slot(0 if dk < 0 else tile_cols + 1)] = jnp.zeros((C, LANE), BF)
                else:
                    edge_in[index, pl.ds(PACK * blocks[side], PACK), :] = jnp.zeros((PACK, tall), BF)

    def edge_picker(first, count):
        row = lax.broadcasted_iota(jnp.int32, (2 * PACK, count * LANE), 0)
        at = lax.broadcasted_iota(jnp.int32, (2 * PACK, count * LANE), 1)
        low = jnp.where(row < PACK, (row - 1 - first) * LANE, (row - PACK - first) * LANE - 1)
        real = jnp.where(row < PACK, row, row - PACK)
        hit = jnp.logical_and(at == low, jnp.logical_and(real > first, real <= first + count))
        return jnp.where(hit, 1.0, 0.0).astype(BF)

    def pad_rows(value):
        return jnp.concatenate([value, jnp.zeros((value.shape[0], tall - C), F32)], axis=1).astype(BF)

    def move(value, by):
        by = by % LANE
        return pltpu.roll(value, by, 1) if by else value

    def preroll(shifts, s, value):
        shifts[0][:, slot(s)] = move(value, 1)
        shifts[2][:, slot(s)] = move(value, -1)

    def mend(shifts, s, halo, low, high):
        before, after = shifts[0][:, slot(s)], shifts[2][:, slot(s)]
        shifts[0][:, slot(s)] = jnp.where(lane == 0, move(halo, -low), before)
        shifts[2][:, slot(s)] = jnp.where(lane == LANE - 1, move(halo, LANE - 1 - high), after)

    def shift(shifts, s, halo, low, high):
        value = shifts[1][:, slot(s)]
        shifts[0][:, slot(s)] = jnp.where(lane == 0, move(halo, -low), move(value, 1))
        shifts[2][:, slot(s)] = jnp.where(
            lane == LANE - 1, move(halo, LANE - 1 - high), move(value, -1)
        )

    def turn(parts):
        have = sum(part.shape[0] for part in parts)
        parts = [part.astype(F32) for part in parts] + [jnp.zeros((LANE - have, tall), F32)]
        return jnp.concatenate(parts, axis=0).T[:C].astype(BF)

    def tile_halo(index, count):
        return turn([edge_in[index, : PACK * count, :]])

    def shift_inner(shifts, s, halo):
        mend(shifts, s, halo, s, PACK + s)

    def shift_ends(shifts, halo):
        shift(shifts, 0, halo, 2 * PACK + tile_cols, 4 * PACK + tile_cols)
        shift(shifts, tile_cols + 1, halo, 3 * PACK + 1, 5 * PACK + 1)

    def control_halo(start, count, outer):
        parts = []
        if count:
            parts.append(cedge_in[pl.ds(pl.multiple_of(PACK * start, PACK), PACK * count), :])
        if outer is not None:
            parts.append(cedge_in[pl.ds(pl.multiple_of(PACK * outer, PACK), PACK), :])
        return turn(parts)

    def shift_control(s, at, halo):
        shift(shifts_c, s, halo, at, at + 1)

    def shift_half(start, halo):
        for c in range(half_cols):
            at = PACK * (c // strip_cols) + 2 * (c % strip_cols)
            shift_control(start + c + 1, at, halo)

    def shift_outer(on_left, at, halo):
        value = jnp.where(on_left == 1, move(halo, -2 * (strip_cols - 1)), halo)
        shift_control((1 - on_left) * (tile_cols + 1), at, value)

    def pack_weights(i):
        for n, t in enumerate(TAPS):
            packed[i, :, pl.ds(n * main, main)] = raw[i, t, :, :main]
        for n in range(0, 9, 2):
            here = raw[i, TAPS[n], :, main:]
            at = 9 * main + n * rest
            if n < 8:
                here = jnp.concatenate([here, raw[i, TAPS[n + 1], :, main:]], axis=1)
            packed[i, :, pl.ds(at, here.shape[1])] = here

    def product(ref, right):
        return jnp.concatenate(
            [
                jnp.dot(ref[:middle, :], right, preferred_element_type=F32),
                jnp.dot(ref[middle:, :], right, preferred_element_type=F32),
            ],
            axis=0,
        )

    def convolve(i, shifts, runs):
        pieces, last = [], []
        for t in TAPS:
            top = [shifts[t % 3][:main, slot(c + t // 3, n)] for c, n in runs]
            low = [shifts[t % 3][main:, slot(c + t // 3, n)] for c, n in runs]
            pieces.append(jnp.concatenate(top, axis=1) if len(top) > 1 else top[0])
            last.append(jnp.concatenate(low, axis=1) if len(low) > 1 else low[0])
        patch = jnp.concatenate(pieces + last, axis=0)
        total = product(packed.at[i], patch)
        count = sum(n for _, n in runs)
        return silu(total + jnp.concatenate([biases[i]] * count, axis=1))

    base_load.wait()
    for w in range(tile_cols):
        b_mid[:, slot(w + 1)] = base[pl.ds(w, C, tile_cols), :].astype(BF)
    edge_out[0] = pad_rows(
        lax.dot_general(
            edge_picker(0, tile_cols),
            b_mid[:, slot(1, tile_cols)],
            NT,
            preferred_element_type=F32,
        )
    )
    pl.semaphore_wait(barrier, peers)
    send_edges(0, shifts_b, ROW_SIDES + WIDE_SIDES)

    def make_strip(q):
        for w in range(strip_cols):
            strips[q, :, w * LANE : (w + 1) * LANE] = flat[
                pl.ds(q * C * strip_cols + w, C, strip_cols), :
            ].astype(BF)

    def strip_copies(q, to, source):
        made = []
        for w in range(strip_cols):
            for i, (low, count) in enumerate(((0, middle), (middle, C - middle))):
                made.append(
                    pltpu.make_async_remote_copy(
                        src_ref=strips.at[q, pl.ds(low, count), slot(w)],
                        dst_ref=c_mid.at[
                            pl.ds(low, count), slot(source * strip_cols + w + 1)
                        ],
                        send_sem=in_send.at[q, w, i],
                        recv_sem=in_recv.at[source, w, i],
                        device_id=(gid, k, to),
                        device_id_type=MESH,
                    )
                )
        return made

    def to_tile(q):
        return strip_copies(q, q, r)

    def from_strip(q):
        return strip_copies(q, q, q)

    def late_sends(step):
        if half > 1:
            for copy in to_tile(fars[-1])[step : 1 if step == 0 else None]:
                copy.start()

    def control_edges(q, to):
        return pltpu.make_async_remote_copy(
            src_ref=cedge_out.at[q],
            dst_ref=cedge_in.at[pl.ds(pl.multiple_of(PACK * (1 + to), PACK), PACK), :],
            send_sem=ce_send.at[q],
            recv_sem=ce_recv.at[to],
            device_id=(gid, k, q),
            device_id_type=MESH,
        )

    def forward(i):
        to_left = far_is_left if i else 1 - far_is_left
        step = 1 - 2 * to_left
        src_slot = 1 + (1 - to_left) * (tile_cols - 1)
        dst_slot = to_left * (tile_cols + 1)
        src_block = 1 + (1 - to_left) * (n_rows - 1)
        dst_block = to_left * (n_rows + 1)
        made = (
            pltpu.make_async_remote_copy(
                src_ref=c_mid.at[:, slot(src_slot)],
                dst_ref=c_mid.at[:, slot(dst_slot)],
                send_sem=fw_send.at[i, 0],
                recv_sem=fw_recv.at[i, 0],
                device_id=(gid, k + step, r),
                device_id_type=MESH,
            ),
            pltpu.make_async_remote_copy(
                src_ref=cedge_in.at[pl.ds(pl.multiple_of(PACK * src_block, PACK), PACK), :],
                dst_ref=cedge_in.at[pl.ds(pl.multiple_of(PACK * dst_block, PACK), PACK), :],
                send_sem=fw_send.at[i, 1],
                recv_sem=fw_recv.at[i, 1],
                device_id=(gid, k + step, r),
                device_id_type=MESH,
            ),
        )
        goes = jnp.where(to_left == 1, k > 0, k < n_cols - 1)
        comes = jnp.where(to_left == 1, k < n_cols - 1, k > 0)
        return made, goes, comes

    def forward_start(i):
        made, goes, _ = forward(i)

        @pl.when(goes)
        def _():
            for copy in made:
                copy.start()

    def forward_recv(i):
        made, _, comes = forward(i)

        @pl.when(comes)
        def _():
            for copy in made:
                copy.wait_recv()

    def forward_sent(i):
        made, goes, _ = forward(i)

        @pl.when(goes)
        def _():
            for copy in made:
                copy.wait_send()

    def to_strip(q, source):
        return pltpu.make_async_remote_copy(
            src_ref=bracket.at[q],
            dst_ref=arrived.at[source],
            send_sem=out_send.at[q],
            recv_sem=out_recv.at[source],
            device_id=(gid, k, q),
            device_id_type=MESH,
        )

    for copy in ctl_loads:
        copy.wait()
    for q in fars:
        make_strip(q)
    for copy in to_tile(fars[0]):
        copy.start()
    for q in buddies:
        make_strip(q)
        for copy in to_tile(q):
            copy.start()
    make_strip(r)
    c_mid[:, slot(r * strip_cols + 1, strip_cols)] = strips[r]

    row = lax.broadcasted_iota(jnp.int32, (2 * PACK, wide), 0)
    at = lax.broadcasted_iota(jnp.int32, (2 * PACK, wide), 1)
    real = jnp.where(row < PACK, row, row - PACK)
    w_of = lax.div(real, 2)
    want = jnp.where(row < PACK, w_of * LANE + LANE - 1, w_of * LANE)
    parity = jnp.where(row < PACK, 0, 1)
    hit = jnp.logical_and(at == want, jnp.logical_and(lax.rem(real, 2) == parity, w_of < strip_cols))
    picker = jnp.where(hit, 1.0, 0.0).astype(BF)
    found = [
        lax.dot_general(picker, strips[q], NT, preferred_element_type=F32) for q in range(n_rows)
    ]
    for q in range(n_rows):
        value = None
        if q > 0:
            value = found[q - 1][:PACK]
        if q < n_rows - 1:
            value = found[q + 1][PACK:] if value is None else value + found[q + 1][PACK:]
        cedge_out[q] = pad_rows(value)
    for q in buddies + fars:
        control_edges(q, r).start()
    cedge_in[pl.ds(pl.multiple_of(PACK * (1 + r), PACK), PACK), :] = cedge_out[r]
    for q in fars[1:-1]:
        for copy in to_tile(q):
            copy.start()
    for copy in row_loads:
        copy.wait()
    for i, ref in enumerate((row1, row2, row3)):
        line = jnp.concatenate([ref[...][None], jnp.zeros((1, tall - C), F32)], axis=1)
        biases[i] = jnp.broadcast_to(line, (LANE, tall)).T[:C]
    clear_edges(0, shifts_b, ROW_SIDES + WIDE_SIDES)
    clear_edges(1, shifts_h, ROW_SIDES)
    clear_edges(2, shifts_h, ROW_SIDES + WIDE_SIDES)

    @pl.when(k == 0)
    def _():
        c_mid[:, slot(0)] = jnp.zeros((C, LANE), BF)
        cedge_in[pl.ds(0, PACK), :] = jnp.zeros((PACK, tall), BF)

    @pl.when(k == n_cols - 1)
    def _():
        c_mid[:, slot(tile_cols + 1)] = jnp.zeros((C, LANE), BF)
        cedge_in[pl.ds(PACK * (n_rows + 1), PACK), :] = jnp.zeros((PACK, tall), BF)

    weight_loads[0].wait()
    pack_weights(0)
    for w in range(tile_cols):
        preroll(shifts_b, w + 1, b_mid[:, slot(w + 1)])

    def hidden(runs):
        value = convolve(0, shifts_b, runs).astype(BF)
        total, done = None, 0
        for c, n in runs:
            here = value[:, done * LANE : (done + n) * LANE]
            h_mid[:, slot(c + 1, n)] = here
            for w in range(n):
                preroll(shifts_h, c + 1 + w, here[:, w * LANE : (w + 1) * LANE])
            part = lax.dot_general(edge_picker(c, n), here, NT, preferred_element_type=F32)
            total = part if total is None else total + part
            done += n
        return total

    inner_start = inward[0] * strip_cols

    await_edges(0, shifts_b, ROW_SIDES)
    late_sends(0)
    for q in buddies:
        for copy in from_strip(q):
            copy.wait_recv()
        control_edges(q, q).wait_recv()
    forward_start(0)
    halo = tile_halo(0, 2)
    ready, edges, c = 1, None, 1
    while c < tile_cols - 1:
        take = min(strip_cols, tile_cols - 1 - c)
        while ready < c + take + 2:
            shift_inner(shifts_b, ready, halo)
            ready += 1
        part = hidden([(c, take)])
        edges = part if edges is None else edges + part
        c += take
    edge_out[1] = pad_rows(edges)
    send_edges(1, shifts_h, ROW_SIDES)
    late_sends(1)

    await_edges(0, shifts_b, WIDE_SIDES)
    shift_ends(shifts_b, tile_halo(0, 6))
    edge_out[2] = pad_rows(hidden([(0, 1), (tile_cols - 1, 1)]))
    send_edges(2, shifts_h, ROW_SIDES + WIDE_SIDES)

    for i in (1, 2):
        weight_loads[i].wait()
    for i in (1, 2):
        pack_weights(i)
    shift_half(near_start, control_halo(1 + near_base, half, None))
    for copy in t_loads:
        copy.wait()

    def second(start):
        own = jnp.concatenate(
            [base[pl.ds(start + w, C, tile_cols), :] for w in range(strip_cols)], axis=1
        )
        mid[:, slot(start, strip_cols)] = convolve(1, shifts_h, [(start, strip_cols)]) + own

    def columns(ref, runs):
        parts = [ref[:, slot(c, n)] for c, n in runs]
        return jnp.concatenate(parts, axis=1) if len(parts) > 1 else parts[0]

    def change_of(middle, runs):
        return middle + product(tc_ref, columns(mid, runs).astype(BF))

    def put_base(change, runs):
        control = columns(c_mid, [(c + 1, n) for c, n in runs]).astype(F32)
        value = columns(mid, runs) + product(tb_ref, (change + control).astype(BF))
        done = 0
        for c, n in runs:
            for w in range(n):
                base_new[pl.ds(c + w, C, tile_cols), :] = value[:, done * LANE : (done + 1) * LANE]
                done += 1

    inner = []
    left = half_cols - 2
    while left > 0:
        take = min(left, strip_cols)
        inner.append([(near_start + half_cols - 1 - left, take)])
        left -= take

    def far_part(j):
        q = inward[j]
        runs = [(q * strip_cols, strip_cols)]
        change = change_of(convolve(2, shifts_c, runs), runs)
        bracket[q] = change.astype(BF)
        to_strip(q, r).start()
        far_change[j] = change

    def far_arrive():
        for q in fars:
            for copy in from_strip(q):
                copy.wait_recv()
            control_edges(q, q).wait_recv()
        forward_start(1)
        shift_half(far_start, control_halo(1 + far_base, half, None))

    def near_inner():
        for i, runs in enumerate(inner):
            inner_mid[i, :, : runs[0][1] * LANE] = convolve(2, shifts_c, runs)

    def second_first():
        await_edges(1, shifts_h, ROW_SIDES)
        rolled = pltpu.roll(tile_halo(1, 2), lax.rem(LANE - inner_start, LANE), 1)
        for i in range(strip_cols + 2):
            mend(shifts_h, inner_start + i, rolled, i, PACK + i)
        second(inner_start)

    @pl.when(r == near_base)
    def _():
        far_arrive()
        second_first()
        far_part(0)
        near_inner()

    @pl.when(r != near_base)
    def _():
        second_first()
        near_inner()
        far_arrive()
        far_part(0)

    await_edges(2, shifts_h, ROW_SIDES + WIDE_SIDES)
    rest_start = far_is_left * (strip_cols + 2)
    rolled = pltpu.roll(tile_halo(1, 2), lax.rem(LANE - 2 - rest_start, LANE), 1)
    for i in range(tile_cols - 2 - strip_cols - 2):
        mend(shifts_h, 2 + rest_start + i, rolled, i, PACK + i)
    halo = tile_halo(2, 6)
    shift_inner(shifts_h, 1, halo)
    shift_inner(shifts_h, tile_cols, halo)
    shift_ends(shifts_h, halo)
    for j in range(1, half):
        second(inward[j] * strip_cols)
    forward_recv(0)
    shift_outer(far_is_left, 0, control_halo(0, 0, (1 - far_is_left) * (n_rows + 1)))
    for j in range(1, half):
        far_part(j)
    for j in range(half):
        put_base(far_change[j], [(inward[j] * strip_cols, strip_cols)])

    for i in range(half):
        second((near_base + i) * strip_cols)
    for i, runs in enumerate(inner):
        change = change_of(inner_mid[i, :, : runs[0][1] * LANE], runs)
        for w in range(runs[0][1]):
            col = half_cols - 1 - (half_cols - 2 - i * strip_cols) + w
            bracket[near_base + col // strip_cols, :, slot(col % strip_cols)] = change[
                :, w * LANE : (w + 1) * LANE
            ].astype(BF)
        put_base(change, runs)

    forward_recv(1)
    halo = control_halo(0, 0, far_is_left * (n_rows + 1))
    shift_outer(1 - far_is_left, 0, halo)
    runs = [(near_start, 1), (near_start + half_cols - 1, 1)]
    change = change_of(convolve(2, shifts_c, runs), runs)
    bracket[near_base, :, slot(0)] = change[:, :LANE].astype(BF)
    bracket[near_base + half - 1, :, slot(strip_cols - 1)] = change[:, LANE:].astype(BF)
    for q in buddies:
        to_strip(q, r).start()
    put_base(change, runs)
    arrived[r] = bracket[r]

    def finish(q):
        for w in range(strip_cols):
            where = pl.ds(q * C * strip_cols + w, C, strip_cols)
            flat[where, :] = flat[where, :] + arrived[q, :, slot(w)].astype(F32)

    finish(r)
    for q in buddies + fars:
        to_strip(q, q).wait_recv()
        finish(q)
    await_sent(0, shifts_b, ROW_SIDES + WIDE_SIDES)
    await_sent(1, shifts_h, ROW_SIDES)
    await_sent(2, shifts_h, ROW_SIDES + WIDE_SIDES)
    for i in range(2):
        forward_sent(i)
    for q in buddies + fars:
        for copy in to_tile(q):
            copy.wait_send()
        control_edges(q, r).wait_send()
        to_strip(q, r).wait_send()


def scoped(n_cols, n_rows, *refs):
    strip_cols = refs[11].shape[2]
    pl.run_scoped(
        functools.partial(kernel, n_cols, n_rows, *refs),
        pltpu.SemaphoreType.DMA((9 + n_rows,)),
        pltpu.SemaphoreType.DMA((3, 8)),
        pltpu.SemaphoreType.DMA((3, 8)),
        pltpu.SemaphoreType.DMA((n_rows, strip_cols, 2)),
        pltpu.SemaphoreType.DMA((n_rows, strip_cols, 2)),
        pltpu.SemaphoreType.DMA((n_rows,)),
        pltpu.SemaphoreType.DMA((n_rows,)),
        pltpu.SemaphoreType.DMA((2, 2)),
        pltpu.SemaphoreType.DMA((2, 2)),
        pltpu.SemaphoreType.DMA((n_rows,)),
        pltpu.SemaphoreType.DMA((n_rows,)),
    )


def deliver(base_new, ctl, base_out, control_out, sem):
    n_rows = ctl.shape[0]
    copies = [pltpu.make_async_copy(base_new, base_out, sem.at[n_rows])]
    for q in range(n_rows):
        copies.append(
            pltpu.make_async_copy(
                ctl.at[q], control_out.at[:, :, pl.ds(q * LANE, LANE)], sem.at[q]
            )
        )
    for copy in copies:
        copy.start()
    for copy in copies:
        copy.wait()


def solution(mesh):
    n_cols, n_rows = mesh.shape["cols"], mesh.shape["rows"]

    def per_device(base, control, k1, k2, kc, b1, b2, bc, tc, tb):
        C, tile_cols, _ = base.shape
        strip_cols = control.shape[1]
        wide = strip_cols * LANE
        tall = -(-C // LANE) * LANE
        area = tile_cols * LANE
        half = n_rows // 2
        held = pltpu.VMEM((C, area + 2 * LANE), BF)
        inner = max(1, -(-(half * strip_cols - 2) // strip_cols))
        hbm = pl.BlockSpec(memory_space=pltpu.HBM)
        vmem = pl.BlockSpec(memory_space=pltpu.VMEM)
        base_new, ctl = pl.pallas_call(
            functools.partial(scoped, n_cols, n_rows),
            out_shape=(
                pltpu.VMEM((C * tile_cols, LANE), F32),
                pltpu.VMEM((n_rows, C, strip_cols, LANE), F32),
            ),
            in_specs=[hbm] * 10,
            out_specs=(vmem, vmem),
            scratch_shapes=[
                pltpu.VMEM((C * tile_cols, LANE), F32),
                pltpu.VMEM((3,) + k1.shape, BF),
                pltpu.VMEM((3, C, 9 * C), BF),
                *[held] * 9,
                pltpu.VMEM((C,), F32),
                pltpu.VMEM((C,), F32),
                pltpu.VMEM((C,), F32),
                pltpu.VMEM((3, C, LANE), F32),
                pltpu.VMEM((C, C), BF),
                pltpu.VMEM((C, C), BF),
                pltpu.VMEM((3, 2 * PACK, tall), BF),
                pltpu.VMEM((3, LANE, tall), BF),
                pltpu.VMEM((n_rows, PACK, tall), BF),
                pltpu.VMEM((LANE, tall), BF),
                pltpu.VMEM((n_rows, C, wide), BF),
                pltpu.VMEM((C, area), F32),
                pltpu.VMEM((inner, C, wide), F32),
                pltpu.VMEM((half, C, wide), F32),
                pltpu.VMEM((n_rows, C, wide), BF),
                pltpu.VMEM((n_rows, C, wide), BF),
            ],
            compiler_params=pltpu.CompilerParams(
                collective_id=0, has_side_effects=True, vmem_limit_bytes=60 * 1024 * 1024
            ),
        )(base.reshape(C * tile_cols, LANE), control, k1, k2, kc, b1, b2, bc, tc, tb)
        base_out, control_out = pl.pallas_call(
            deliver,
            out_shape=(
                jax.ShapeDtypeStruct(base_new.shape, F32),
                jax.ShapeDtypeStruct(control.shape, F32),
            ),
            in_specs=[vmem] * 2,
            out_specs=(hbm, hbm),
            scratch_shapes=[pltpu.SemaphoreType.DMA((n_rows + 1,))],
            compiler_params=pltpu.CompilerParams(vmem_limit_bytes=1024 * 1024),
        )(base_new, ctl)
        return base_out.reshape(base.shape), control_out

    tiles = P(None, ("groups", "cols"), "rows")
    lines = P(None, ("groups", "cols", "rows"), None)
    return jax.shard_map(
        per_device,
        mesh=mesh,
        in_specs=(tiles, lines) + (P(),) * 8,
        out_specs=(tiles, lines),
        check_vma=False,
    )
```

```python
import functools

import jax
import jax.numpy as jnp
from jax import lax
from jax.experimental import pallas as pl
from jax.experimental.pallas import tpu as pltpu
from jax.sharding import PartitionSpec as P

MESH = pl.DeviceIdType.MESH
BF = jnp.bfloat16
F32 = jnp.float32
LANE = 128
PACK = 16
SIDES = ((-1, 0), (1, 0), (0, -1), (0, 1), (-1, -1), (1, -1), (-1, 1), (1, 1))
ROW_SIDES = ((0, 1), (0, -1))
WIDE_SIDES = tuple(side for side in SIDES if side[0] and side[1]) + ((-1, 0), (1, 0))
TAPS = (1, 4, 7, 0, 3, 6, 2, 5, 8)
NT = (((1,), (1,)), ((), ()))


def silu(v):
    return 0.5 * v * (1.0 + jnp.tanh(0.5 * v))


def kernel(
    n_cols,
    n_rows,
    base_hbm,
    control_hbm,
    k1_hbm,
    k2_hbm,
    kc_hbm,
    b1_hbm,
    b2_hbm,
    bc_hbm,
    tc_hbm,
    tb_hbm,
    base_new,
    ctl,
    base,
    raw,
    packed,
    b_low,
    b_mid,
    b_high,
    h_low,
    h_mid,
    h_high,
    c_low,
    c_mid,
    c_high,
    row1,
    row2,
    row3,
    biases,
    tc_ref,
    tb_ref,
    edge_out,
    edge_in,
    cedge_out,
    cedge_in,
    strips,
    mid,
    inner_mid,
    far_change,
    bracket,
    arrived,
    load_sem,
    x_send,
    x_recv,
    in_send,
    in_recv,
    ce_send,
    ce_recv,
    fw_send,
    fw_recv,
    out_send,
    out_recv,
):
    C = tc_ref.shape[0]
    tile_cols = base.shape[0] // C
    strip_cols = ctl.shape[2]
    wide = strip_cols * LANE
    main = C - C % LANE
    rest = C - main
    tall = edge_out.shape[2]
    half = n_rows // 2
    half_cols = half * strip_cols
    middle = C // 2 // PACK * PACK
    assert n_rows == 2 * half and half_cols == strip_cols + 2 and 2 * half_cols == tile_cols
    gid = lax.axis_index("groups")
    k = lax.axis_index("cols")
    r = lax.axis_index("rows")
    lane = lax.broadcasted_iota(jnp.int32, (C, LANE), 1)
    flat = ctl.reshape(n_rows * C * strip_cols, LANE)

    shifts_b = (b_low, b_mid, b_high)
    shifts_h = (h_low, h_mid, h_high)
    shifts_c = (c_low, c_mid, c_high)
    near_base = half * lax.div(r, half)
    far_base = half - near_base
    far_is_left = lax.div(r, half)
    near_start = near_base * strip_cols
    far_start = far_base * strip_cols
    buddies = [near_base + lax.rem(r - near_base + o, half) for o in range(1, half)]
    fars = [far_base + j + (1 - far_is_left) * (half - 1 - 2 * j) for j in range(half)]
    leads = r == near_base + (half - 1) * far_is_left
    inward = [far_base + j + far_is_left * (half - 1 - 2 * j) for j in range(half)]

    def load(i, src, dst):
        copy = pltpu.make_async_copy(src, dst, load_sem.at[i])
        copy.start()
        return copy

    base_loads = []
    for i, (low, count) in enumerate(((0, middle), (middle, C - middle))):
        rows = pl.ds(low * tile_cols, count * tile_cols)
        base_loads.append((low, count, load(i, base_hbm.at[rows, :], base.at[rows, :])))
    ctl_loads = [
        load(2 + q, control_hbm.at[:, :, pl.ds(q * LANE, LANE)], ctl.at[q]) for q in range(n_rows)
    ]
    more = 2 + n_rows
    weight_loads = [load(more, k1_hbm, raw.at[0])]
    row_loads = [
        load(more + 3 + i, src, dst)
        for i, (src, dst) in enumerate(((b1_hbm, row1), (b2_hbm, row2), (bc_hbm, row3)))
    ]
    weight_loads.append(load(more + 2, kc_hbm, raw.at[2]))
    weight_loads.insert(1, load(more + 1, k2_hbm, raw.at[1]))
    t_loads = [load(more + 6, tc_hbm, tc_ref), load(more + 7, tb_hbm, tb_ref)]

    def there(side):
        dk, dr = side
        ok = None
        for at, step, count in ((k, dk, n_cols), (r, dr, n_rows)):
            if step:
                test = (at > 0) if step < 0 else (at < count - 1)
                ok = test if ok is None else jnp.logical_and(ok, test)
        return ok

    barrier = pltpu.get_barrier_semaphore()
    peers = n_rows - 1
    for side in SIDES:
        if side[0]:
            peers = peers + jnp.where(there(side), 1, 0)

            @pl.when(there(side))
            def _():
                pl.semaphore_signal(
                    barrier, inc=1, device_id=(gid, k + side[0], r + side[1]), device_id_type=MESH
                )
    for o in range(1, n_rows):
        pl.semaphore_signal(
            barrier, inc=1, device_id=(gid, k, lax.rem(r + o, n_rows)), device_id_type=MESH
        )

    def slot(s, count=1):
        at = s * LANE
        if not isinstance(at, int):
            at = pl.multiple_of(at, LANE)
        return pl.ds(at, count * LANE)

    blocks = {(0, -1): 0, (0, 1): 1, (-1, -1): 2, (1, -1): 3, (-1, 1): 4, (1, 1): 5}

    def exchange(index, shifts, which):
        made = []
        for side in which:
            i = SIDES.index(side)
            dk, dr = side
            if dr == 0:
                src = shifts[1].at[:, slot(1 if dk < 0 else tile_cols)]
                dst = shifts[1].at[:, slot(tile_cols + 1 if dk < 0 else 0)]
            else:
                src = edge_out.at[index, pl.ds(0 if dr < 0 else PACK, PACK), :]
                dst = edge_in.at[index, pl.ds(PACK * blocks[(-dk, -dr)], PACK), :]
            made.append(
                pltpu.make_async_remote_copy(
                    src_ref=src,
                    dst_ref=dst,
                    send_sem=x_send.at[index, i],
                    recv_sem=x_recv.at[index, i],
                    device_id=(gid, k + dk, r + dr),
                    device_id_type=MESH,
                )
            )
        return made

    def send_edges(index, shifts, which):
        for side, copy in zip(which, exchange(index, shifts, which)):
            @pl.when(there(side))
            def _():
                copy.start()

    def await_edges(index, shifts, which):
        facing = [(-side[0], -side[1]) for side in which]
        for side, copy in zip(which, exchange(index, shifts, facing)):
            @pl.when(there(side))
            def _():
                copy.wait_recv()

    def await_sent(index, shifts, which):
        for side, copy in zip(which, exchange(index, shifts, which)):
            @pl.when(there(side))
            def _():
                copy.wait_send()

    def clear_edges(index, shifts, which):
        for side in which:
            dk, dr = side

            @pl.when(jnp.logical_not(there(side)))
            def _():
                if dr == 0:
                    shifts[1][:, slot(0 if dk < 0 else tile_cols + 1)] = jnp.zeros((C, LANE), BF)
                else:
                    edge_in[index, pl.ds(PACK * blocks[side], PACK), :] = jnp.zeros((PACK, tall), BF)

    def edge_picker(first, count):
        row = lax.broadcasted_iota(jnp.int32, (2 * PACK, count * LANE), 0)
        at = lax.broadcasted_iota(jnp.int32, (2 * PACK, count * LANE), 1)
        low = jnp.where(row < PACK, (row - 1 - first) * LANE, (row - PACK - first) * LANE - 1)
        real = jnp.where(row < PACK, row, row - PACK)
        hit = jnp.logical_and(at == low, jnp.logical_and(real > first, real <= first + count))
        return jnp.where(hit, 1.0, 0.0).astype(BF)

    def pad_rows(value):
        return jnp.concatenate([value, jnp.zeros((value.shape[0], tall - C), F32)], axis=1).astype(BF)

    def move(value, by):
        by = by % LANE
        return pltpu.roll(value, by, 1) if by else value

    def preroll(shifts, s, value):
        shifts[0][:, slot(s)] = move(value, 1)
        shifts[2][:, slot(s)] = move(value, -1)

    def mend(shifts, s, halo, low, high):
        before, after = shifts[0][:, slot(s)], shifts[2][:, slot(s)]
        shifts[0][:, slot(s)] = jnp.where(lane == 0, move(halo, -low), before)
        shifts[2][:, slot(s)] = jnp.where(lane == LANE - 1, move(halo, LANE - 1 - high), after)

    def shift(shifts, s, halo, low, high):
        value = shifts[1][:, slot(s)]
        shifts[0][:, slot(s)] = jnp.where(lane == 0, move(halo, -low), move(value, 1))
        shifts[2][:, slot(s)] = jnp.where(
            lane == LANE - 1, move(halo, LANE - 1 - high), move(value, -1)
        )

    def turn(parts):
        have = sum(part.shape[0] for part in parts)
        parts = [part.astype(F32) for part in parts] + [jnp.zeros((LANE - have, tall), F32)]
        return jnp.concatenate(parts, axis=0).T[:C].astype(BF)

    def tile_halo(index, count):
        return turn([edge_in[index, : PACK * count, :]])

    def shift_inner(shifts, s, halo):
        mend(shifts, s, halo, s, PACK + s)

    def shift_ends(shifts, halo):
        shift(shifts, 0, halo, 2 * PACK + tile_cols, 4 * PACK + tile_cols)
        shift(shifts, tile_cols + 1, halo, 3 * PACK + 1, 5 * PACK + 1)

    def control_halo(start, count, outer):
        parts = []
        if count:
            parts.append(cedge_in[pl.ds(pl.multiple_of(PACK * start, PACK), PACK * count), :])
        if outer is not None:
            parts.append(cedge_in[pl.ds(pl.multiple_of(PACK * outer, PACK), PACK), :])
        return turn(parts)

    def shift_control(s, at, halo):
        shift(shifts_c, s, halo, at, at + 1)

    def shift_half(start, halo):
        for c in range(half_cols):
            at = PACK * (c // strip_cols) + 2 * (c % strip_cols)
            shift_control(start + c + 1, at, halo)

    def shift_outer(on_left, at, halo):
        value = jnp.where(on_left == 1, move(halo, -2 * (strip_cols - 1)), halo)
        shift_control((1 - on_left) * (tile_cols + 1), at, value)

    def pack_weights(i):
        for n, t in enumerate(TAPS):
            packed[i, :, pl.ds(n * main, main)] = raw[i, t, :, :main]
        for n in range(0, 9, 2):
            here = raw[i, TAPS[n], :, main:]
            at = 9 * main + n * rest
            if n < 8:
                here = jnp.concatenate([here, raw[i, TAPS[n + 1], :, main:]], axis=1)
            packed[i, :, pl.ds(at, here.shape[1])] = here

    def product(ref, right):
        return jnp.concatenate(
            [
                jnp.dot(ref[:middle, :], right, preferred_element_type=F32),
                jnp.dot(ref[middle:, :], right, preferred_element_type=F32),
            ],
            axis=0,
        )

    def convolve(i, shifts, runs):
        pieces, last = [], []
        for t in TAPS:
            top = [shifts[t % 3][:main, slot(c + t // 3, n)] for c, n in runs]
            low = [shifts[t % 3][main:, slot(c + t // 3, n)] for c, n in runs]
            pieces.append(jnp.concatenate(top, axis=1) if len(top) > 1 else top[0])
            last.append(jnp.concatenate(low, axis=1) if len(low) > 1 else low[0])
        patch = jnp.concatenate(pieces + last, axis=0)
        total = product(packed.at[i], patch)
        count = sum(n for _, n in runs)
        return silu(total + jnp.concatenate([biases[i]] * count, axis=1))

    for low, count, copy in base_loads:
        copy.wait()
        for w in range(tile_cols):
            b_mid[low : low + count, slot(w + 1)] = base[
                pl.ds(low * tile_cols + w, count, tile_cols), :
            ].astype(BF)
    edge_out[0] = pad_rows(
        lax.dot_general(
            edge_picker(0, tile_cols),
            b_mid[:, slot(1, tile_cols)],
            NT,
            preferred_element_type=F32,
        )
    )
    pl.semaphore_wait(barrier, peers)
    send_edges(0, shifts_b, ROW_SIDES + WIDE_SIDES)

    def make_strip(q):
        for w in range(strip_cols):
            strips[q, :, w * LANE : (w + 1) * LANE] = flat[
                pl.ds(q * C * strip_cols + w, C, strip_cols), :
            ].astype(BF)

    def strip_copies(q, to, source):
        made = []
        for w in range(strip_cols):
            for i, (low, count) in enumerate(((0, middle), (middle, C - middle))):
                made.append(
                    pltpu.make_async_remote_copy(
                        src_ref=strips.at[q, pl.ds(low, count), slot(w)],
                        dst_ref=c_mid.at[
                            pl.ds(low, count), slot(source * strip_cols + w + 1)
                        ],
                        send_sem=in_send.at[q, w, i],
                        recv_sem=in_recv.at[source, w, i],
                        device_id=(gid, k, to),
                        device_id_type=MESH,
                    )
                )
        return made

    def to_tile(q):
        return strip_copies(q, q, r)

    def from_strip(q):
        return strip_copies(q, q, q)

    def late_sends(step):
        if half > 1:
            for copy in to_tile(fars[-1])[step * strip_cols : (step + 1) * strip_cols]:
                copy.start()

    def control_edges(q, to):
        return pltpu.make_async_remote_copy(
            src_ref=cedge_out.at[q],
            dst_ref=cedge_in.at[pl.ds(pl.multiple_of(PACK * (1 + to), PACK), PACK), :],
            send_sem=ce_send.at[q],
            recv_sem=ce_recv.at[to],
            device_id=(gid, k, q),
            device_id_type=MESH,
        )

    def forward(i):
        to_left = far_is_left if i else 1 - far_is_left
        step = 1 - 2 * to_left
        src_slot = 1 + (1 - to_left) * (tile_cols - 1)
        dst_slot = to_left * (tile_cols + 1)
        src_block = 1 + (1 - to_left) * (n_rows - 1)
        dst_block = to_left * (n_rows + 1)
        made = (
            pltpu.make_async_remote_copy(
                src_ref=c_mid.at[:, slot(src_slot)],
                dst_ref=c_mid.at[:, slot(dst_slot)],
                send_sem=fw_send.at[i, 0],
                recv_sem=fw_recv.at[i, 0],
                device_id=(gid, k + step, r),
                device_id_type=MESH,
            ),
            pltpu.make_async_remote_copy(
                src_ref=cedge_in.at[pl.ds(pl.multiple_of(PACK * src_block, PACK), PACK), :],
                dst_ref=cedge_in.at[pl.ds(pl.multiple_of(PACK * dst_block, PACK), PACK), :],
                send_sem=fw_send.at[i, 1],
                recv_sem=fw_recv.at[i, 1],
                device_id=(gid, k + step, r),
                device_id_type=MESH,
            ),
        )
        goes = jnp.where(to_left == 1, k > 0, k < n_cols - 1)
        comes = jnp.where(to_left == 1, k < n_cols - 1, k > 0)
        return made, goes, comes

    def forward_start(i):
        made, goes, _ = forward(i)

        @pl.when(goes)
        def _():
            for copy in made:
                copy.start()

    def forward_recv(i):
        made, _, comes = forward(i)

        @pl.when(comes)
        def _():
            for copy in made:
                copy.wait_recv()

    def forward_sent(i):
        made, goes, _ = forward(i)

        @pl.when(goes)
        def _():
            for copy in made:
                copy.wait_send()

    def to_strip(q, source):
        return pltpu.make_async_remote_copy(
            src_ref=bracket.at[q],
            dst_ref=arrived.at[source],
            send_sem=out_send.at[q],
            recv_sem=out_recv.at[source],
            device_id=(gid, k, q),
            device_id_type=MESH,
        )

    for copy in ctl_loads:
        copy.wait()
    for q in fars:
        make_strip(q)
    for copy in to_tile(fars[0]):
        copy.start()
    for q in buddies:
        make_strip(q)
        for copy in to_tile(q):
            copy.start()
    make_strip(r)
    c_mid[:, slot(r * strip_cols + 1, strip_cols)] = strips[r]

    row = lax.broadcasted_iota(jnp.int32, (2 * PACK, wide), 0)
    at = lax.broadcasted_iota(jnp.int32, (2 * PACK, wide), 1)
    real = jnp.where(row < PACK, row, row - PACK)
    w_of = lax.div(real, 2)
    want = jnp.where(row < PACK, w_of * LANE + LANE - 1, w_of * LANE)
    parity = jnp.where(row < PACK, 0, 1)
    hit = jnp.logical_and(at == want, jnp.logical_and(lax.rem(real, 2) == parity, w_of < strip_cols))
    picker = jnp.where(hit, 1.0, 0.0).astype(BF)
    found = [
        lax.dot_general(picker, strips[q], NT, preferred_element_type=F32) for q in range(n_rows)
    ]
    for q in range(n_rows):
        value = None
        if q > 0:
            value = found[q - 1][:PACK]
        if q < n_rows - 1:
            value = found[q + 1][PACK:] if value is None else value + found[q + 1][PACK:]
        cedge_out[q] = pad_rows(value)
    for q in buddies + fars:
        control_edges(q, r).start()
    cedge_in[pl.ds(pl.multiple_of(PACK * (1 + r), PACK), PACK), :] = cedge_out[r]
    for q in fars[1:-1]:
        for copy in to_tile(q):
            copy.start()
    for copy in row_loads:
        copy.wait()
    for i, ref in enumerate((row1, row2, row3)):
        line = jnp.concatenate([ref[...][None], jnp.zeros((1, tall - C), F32)], axis=1)
        biases[i] = jnp.broadcast_to(line, (LANE, tall)).T[:C]
    clear_edges(0, shifts_b, ROW_SIDES + WIDE_SIDES)
    clear_edges(1, shifts_h, ROW_SIDES)
    clear_edges(2, shifts_h, ROW_SIDES + WIDE_SIDES)

    @pl.when(k == 0)
    def _():
        c_mid[:, slot(0)] = jnp.zeros((C, LANE), BF)
        cedge_in[pl.ds(0, PACK), :] = jnp.zeros((PACK, tall), BF)

    @pl.when(k == n_cols - 1)
    def _():
        c_mid[:, slot(tile_cols + 1)] = jnp.zeros((C, LANE), BF)
        cedge_in[pl.ds(PACK * (n_rows + 1), PACK), :] = jnp.zeros((PACK, tall), BF)

    weight_loads[0].wait()
    pack_weights(0)
    for w in range(tile_cols):
        preroll(shifts_b, w + 1, b_mid[:, slot(w + 1)])

    def hidden(runs):
        value = convolve(0, shifts_b, runs).astype(BF)
        total, done = None, 0
        for c, n in runs:
            here = value[:, done * LANE : (done + n) * LANE]
            h_mid[:, slot(c + 1, n)] = here
            for w in range(n):
                preroll(shifts_h, c + 1 + w, here[:, w * LANE : (w + 1) * LANE])
            part = lax.dot_general(edge_picker(c, n), here, NT, preferred_element_type=F32)
            total = part if total is None else total + part
            done += n
        return total

    inner_start = inward[0] * strip_cols

    await_edges(0, shifts_b, ROW_SIDES)
    late_sends(0)
    for q in buddies:
        for copy in from_strip(q):
            copy.wait_recv()
        control_edges(q, q).wait_recv()
    forward_start(0)
    halo = tile_halo(0, 2)
    ready, edges, c = 1, None, 1
    while c < tile_cols - 1:
        take = min(strip_cols, tile_cols - 1 - c)
        while ready < c + take + 2:
            shift_inner(shifts_b, ready, halo)
            ready += 1
        part = hidden([(c, take)])
        edges = part if edges is None else edges + part
        c += take
    edge_out[1] = pad_rows(edges)
    send_edges(1, shifts_h, ROW_SIDES)
    late_sends(1)

    await_edges(0, shifts_b, WIDE_SIDES)
    shift_ends(shifts_b, tile_halo(0, 6))
    edge_out[2] = pad_rows(hidden([(0, 1), (tile_cols - 1, 1)]))
    send_edges(2, shifts_h, ROW_SIDES + WIDE_SIDES)

    for i in (1, 2):
        weight_loads[i].wait()
    for i in (1, 2):
        pack_weights(i)
    shift_half(near_start, control_halo(1 + near_base, half, None))
    for copy in t_loads:
        copy.wait()

    def second(start):
        own = jnp.concatenate(
            [base[pl.ds(start + w, C, tile_cols), :] for w in range(strip_cols)], axis=1
        )
        mid[:, slot(start, strip_cols)] = convolve(1, shifts_h, [(start, strip_cols)]) + own

    def columns(ref, runs):
        parts = [ref[:, slot(c, n)] for c, n in runs]
        return jnp.concatenate(parts, axis=1) if len(parts) > 1 else parts[0]

    def change_of(middle, runs):
        return middle + product(tc_ref, columns(mid, runs).astype(BF))

    def put_base(change, runs):
        control = columns(c_mid, [(c + 1, n) for c, n in runs]).astype(F32)
        value = columns(mid, runs) + product(tb_ref, (change + control).astype(BF))
        done = 0
        for c, n in runs:
            for w in range(n):
                base_new[pl.ds(c + w, C, tile_cols), :] = value[:, done * LANE : (done + 1) * LANE]
                done += 1

    inner = []
    left = half_cols - 2
    while left > 0:
        take = min(left, strip_cols)
        inner.append([(near_start + half_cols - 1 - left, take)])
        left -= take

    def far_part(j):
        q = inward[j]
        runs = [(q * strip_cols, strip_cols)]
        change = change_of(convolve(2, shifts_c, runs), runs)
        bracket[q] = change.astype(BF)
        to_strip(q, r).start()
        far_change[j] = change

    def far_arrive():
        for q in fars:
            for copy in from_strip(q):
                copy.wait_recv()
            control_edges(q, q).wait_recv()
        forward_start(1)
        shift_half(far_start, control_halo(1 + far_base, half, None))

    def near_inner():
        for i, runs in enumerate(inner):
            inner_mid[i, :, : runs[0][1] * LANE] = convolve(2, shifts_c, runs)

    def second_first():
        await_edges(1, shifts_h, ROW_SIDES)
        rolled = pltpu.roll(tile_halo(1, 2), lax.rem(LANE - inner_start, LANE), 1)
        for i in range(strip_cols + 2):
            mend(shifts_h, inner_start + i, rolled, i, PACK + i)
        second(inner_start)

    @pl.when(leads)
    def _():
        far_arrive()
        second_first()
        far_part(0)
        near_inner()

    @pl.when(jnp.logical_not(leads))
    def _():
        second_first()
        near_inner()
        far_arrive()
        far_part(0)

    await_edges(2, shifts_h, ROW_SIDES + WIDE_SIDES)
    rest_start = far_is_left * (strip_cols + 2)
    rolled = pltpu.roll(tile_halo(1, 2), lax.rem(LANE - 2 - rest_start, LANE), 1)
    for i in range(tile_cols - 2 - strip_cols - 2):
        mend(shifts_h, 2 + rest_start + i, rolled, i, PACK + i)
    halo = tile_halo(2, 6)
    shift_inner(shifts_h, 1, halo)
    shift_inner(shifts_h, tile_cols, halo)
    shift_ends(shifts_h, halo)
    for j in range(1, half):
        second(inward[j] * strip_cols)
    forward_recv(0)
    shift_outer(far_is_left, 0, control_halo(0, 0, (1 - far_is_left) * (n_rows + 1)))
    for j in range(1, half):
        far_part(j)
    for j in range(half):
        put_base(far_change[j], [(inward[j] * strip_cols, strip_cols)])

    for i in range(half):
        second((near_base + i) * strip_cols)
    for i, runs in enumerate(inner):
        change = change_of(inner_mid[i, :, : runs[0][1] * LANE], runs)
        for w in range(runs[0][1]):
            col = half_cols - 1 - (half_cols - 2 - i * strip_cols) + w
            bracket[near_base + col // strip_cols, :, slot(col % strip_cols)] = change[
                :, w * LANE : (w + 1) * LANE
            ].astype(BF)
        put_base(change, runs)

    forward_recv(1)
    halo = control_halo(0, 0, far_is_left * (n_rows + 1))
    shift_outer(1 - far_is_left, 0, halo)
    runs = [(near_start, 1), (near_start + half_cols - 1, 1)]
    change = change_of(convolve(2, shifts_c, runs), runs)
    bracket[near_base, :, slot(0)] = change[:, :LANE].astype(BF)
    bracket[near_base + half - 1, :, slot(strip_cols - 1)] = change[:, LANE:].astype(BF)
    for q in buddies:
        to_strip(q, r).start()
    put_base(change, runs)
    arrived[r] = bracket[r]

    def finish(q):
        for w in range(strip_cols):
            where = pl.ds(q * C * strip_cols + w, C, strip_cols)
            flat[where, :] = flat[where, :] + arrived[q, :, slot(w)].astype(F32)

    finish(r)
    for q in buddies + fars:
        to_strip(q, q).wait_recv()
        finish(q)
    await_sent(0, shifts_b, ROW_SIDES + WIDE_SIDES)
    await_sent(1, shifts_h, ROW_SIDES)
    await_sent(2, shifts_h, ROW_SIDES + WIDE_SIDES)
    for i in range(2):
        forward_sent(i)
    for q in buddies + fars:
        for copy in to_tile(q):
            copy.wait_send()
        control_edges(q, r).wait_send()
        to_strip(q, r).wait_send()


def scoped(n_cols, n_rows, *refs):
    strip_cols = refs[11].shape[2]
    pl.run_scoped(
        functools.partial(kernel, n_cols, n_rows, *refs),
        pltpu.SemaphoreType.DMA((10 + n_rows,)),
        pltpu.SemaphoreType.DMA((3, 8)),
        pltpu.SemaphoreType.DMA((3, 8)),
        pltpu.SemaphoreType.DMA((n_rows, strip_cols, 2)),
        pltpu.SemaphoreType.DMA((n_rows, strip_cols, 2)),
        pltpu.SemaphoreType.DMA((n_rows,)),
        pltpu.SemaphoreType.DMA((n_rows,)),
        pltpu.SemaphoreType.DMA((2, 2)),
        pltpu.SemaphoreType.DMA((2, 2)),
        pltpu.SemaphoreType.DMA((n_rows,)),
        pltpu.SemaphoreType.DMA((n_rows,)),
    )


def deliver(base_new, ctl, base_out, control_out):
    def body(sem):
        n_rows = ctl.shape[0]
        step = base_new.shape[0] // n_rows
        copies = []
        for q in range(n_rows):
            rows = pl.ds(q * step, step)
            copies.append((base_new.at[rows, :], base_out.at[rows, :]))
            copies.append((ctl.at[q], control_out.at[:, :, pl.ds(q * LANE, LANE)]))
        copies = [
            pltpu.make_async_copy(src, dst, sem.at[i]) for i, (src, dst) in enumerate(copies)
        ]
        for copy in copies:
            copy.start()
        for copy in copies:
            copy.wait()

    pl.run_scoped(body, pltpu.SemaphoreType.DMA((2 * ctl.shape[0],)))


def solution(mesh):
    n_cols, n_rows = mesh.shape["cols"], mesh.shape["rows"]

    def per_device(base, control, k1, k2, kc, b1, b2, bc, tc, tb):
        C, tile_cols, _ = base.shape
        strip_cols = control.shape[1]
        wide = strip_cols * LANE
        tall = -(-C // LANE) * LANE
        area = tile_cols * LANE
        half = n_rows // 2
        held = pltpu.VMEM((C, area + 2 * LANE), BF)
        inner = max(1, -(-(half * strip_cols - 2) // strip_cols))
        hbm = pl.BlockSpec(memory_space=pltpu.HBM)
        vmem = pl.BlockSpec(memory_space=pltpu.VMEM)
        base_new, ctl = pl.pallas_call(
            functools.partial(scoped, n_cols, n_rows),
            out_shape=(
                pltpu.VMEM((C * tile_cols, LANE), F32),
                pltpu.VMEM((n_rows, C, strip_cols, LANE), F32),
            ),
            in_specs=[hbm] * 10,
            out_specs=(vmem, vmem),
            scratch_shapes=[
                pltpu.VMEM((C * tile_cols, LANE), F32),
                pltpu.VMEM((3,) + k1.shape, BF),
                pltpu.VMEM((3, C, 9 * C), BF),
                *[held] * 9,
                pltpu.VMEM((C,), F32),
                pltpu.VMEM((C,), F32),
                pltpu.VMEM((C,), F32),
                pltpu.VMEM((3, C, LANE), F32),
                pltpu.VMEM((C, C), BF),
                pltpu.VMEM((C, C), BF),
                pltpu.VMEM((3, 2 * PACK, tall), BF),
                pltpu.VMEM((3, LANE, tall), BF),
                pltpu.VMEM((n_rows, PACK, tall), BF),
                pltpu.VMEM((LANE, tall), BF),
                pltpu.VMEM((n_rows, C, wide), BF),
                pltpu.VMEM((C, area), F32),
                pltpu.VMEM((inner, C, wide), F32),
                pltpu.VMEM((half, C, wide), F32),
                pltpu.VMEM((n_rows, C, wide), BF),
                pltpu.VMEM((n_rows, C, wide), BF),
            ],
            compiler_params=pltpu.CompilerParams(
                collective_id=0, has_side_effects=True, vmem_limit_bytes=60 * 1024 * 1024
            ),
        )(base.reshape(C * tile_cols, LANE), control, k1, k2, kc, b1, b2, bc, tc, tb)
        base_out, control_out = pl.pallas_call(
            deliver,
            out_shape=(
                jax.ShapeDtypeStruct(base_new.shape, F32),
                jax.ShapeDtypeStruct(control.shape, F32),
            ),
            in_specs=[vmem] * 2,
            out_specs=(hbm, hbm),
            compiler_params=pltpu.CompilerParams(vmem_limit_bytes=1024 * 1024),
        )(base_new, ctl)
        return base_out.reshape(base.shape), control_out

    tiles = P(None, ("groups", "cols"), "rows")
    lines = P(None, ("groups", "cols", "rows"), None)
    return jax.shard_map(
        per_device,
        mesh=mesh,
        in_specs=(tiles, lines) + (P(),) * 8,
        out_specs=(tiles, lines),
        check_vma=False,
    )
```
